128 devices in a mesh: role: 2 (over core), shard: 64 (over y, z, x).
Axes of the slice: x: 4, y: 4, z: 4, core: 2. Of those that a mesh axis runs over, the one named last changes fastest.
Arguments:
- history: bfloat16 [1024, 2560, 128], P(None, ('role', 'shard')), may hold values from -20 to 20
- event_cat: int32 [1024, 2560], P(None, ('role', 'shard')), may hold values from 0 to 1023, as said below
- candidates: bfloat16 [1024, 200, 128], P(('role', 'shard')), may hold values from -9 to 9
- cand_cat: int32 [1024, 200], P(('role', 'shard')), may hold values from 0 to 1023, as said below
- w_input: bfloat16 [256, 512], replicated, may hold values from -0.375 to 0.375
- w_output: bfloat16 [512, 128], replicated, may hold values from -0.25 to 0.25
Outputs:
- interest_features: bfloat16 [1024, 200, 128], P(('role', 'shard'))
The draws below stay inside these ranges and needn't reach their ends.
Inputs may be any that keep to these rules, and one draw needn't show every extreme that they name: `event_cat`: in each aligned block of 20 events of one user, at most 8 events have a category that some candidate of that user has; users 2 i and 2 i + 1 have exactly 8 such events together in every block; every user has a block with exactly 8. `cand_cat`: the candidates of one user carry at most 8 distinct categories.
All inputs are finite; a program needn't handle non-finite values.
Results may differ from the reference program's by a relative error of at most 0.0095.
Values may be sent and summed in bfloat16 or wider, within the bound.
A program may use at most 64 MiB of HBM per device.

```python
import math
import jax
import jax.numpy as jnp
from jax import lax

D = 128
HEADS = 4
HID = 512
NCAT = 1024
CANDS = 200
QCAT = 8
CAP = 8
E_DEV = 20
USERS = 1024
EVENTS = 2560


def user_base(key):
    return jax.random.randint(jax.random.fold_in(key, 101), (USERS,), 0, NCAT)


def draw_cand_cat(key, part):
    base = user_base(key)
    user_keys = jax.random.split(jax.random.fold_in(key, 111), USERS)
    orders = jax.vmap(lambda single: jax.random.permutation(single, CANDS))(user_keys)
    inverse = jnp.argsort(orders, axis=1).astype(jnp.int32)
    picked = jax.random.randint(jax.random.fold_in(key, 112), (USERS, CANDS), 0, QCAT)
    offset = jnp.where(inverse < QCAT, inverse, picked)
    return ((base[:, None] + offset) % NCAT).astype(jnp.int32)


def draw_event_cat(key, part):
    base = user_base(key)
    blocks = EVENTS // E_DEV
    pairs = USERS // 2
    first = jax.random.randint(jax.random.fold_in(key, 121), (pairs, blocks), 0, CAP + 1)
    full_block = jax.random.randint(jax.random.fold_in(key, 122), (pairs,), 0, blocks)
    empty_block = (full_block + 1 + jax.random.randint(jax.random.fold_in(key, 126), (pairs,), 0, blocks - 1)) % blocks
    block_ids = jnp.arange(blocks)[None, :]
    first = jnp.where(block_ids == full_block[:, None], CAP, first)
    first = jnp.where(block_ids == empty_block[:, None], 0, first)
    counts = jnp.stack([first, CAP - first], axis=1).reshape(USERS, blocks)
    block_keys = jax.random.split(jax.random.fold_in(key, 123), USERS * blocks)
    orders = jax.vmap(lambda single: jax.random.permutation(single, E_DEV))(block_keys).reshape(USERS, blocks, E_DEV)
    matched = orders < counts[:, :, None]
    inside = jax.random.randint(jax.random.fold_in(key, 124), (USERS, blocks, E_DEV), 0, QCAT)
    outside = jax.random.randint(jax.random.fold_in(key, 125), (USERS, blocks, E_DEV), QCAT, NCAT)
    offset = jnp.where(matched, inside, outside)
    return ((base[:, None, None] + offset) % NCAT).reshape(USERS, EVENTS).astype(jnp.int32)


def draw_history(key, part):
    noise_key = jax.random.fold_in(key, 303)

    def one_user(index):
        single = jax.random.fold_in(noise_key, index)
        noise = jnp.clip(jax.random.normal(single, (EVENTS, D), jnp.float32), -6.0, 6.0)
        return noise.astype(jnp.bfloat16)
    return lax.map(one_user, jnp.arange(USERS, dtype=jnp.int32))


def draw_candidates(key, part):
    values = jnp.clip(1.5 * jax.random.normal(jax.random.fold_in(key, 404), (USERS, CANDS, D), jnp.float32), -9.0, 9.0)
    return values.astype(jnp.bfloat16)


def scatter_about(own_key, extent, scale, reach, kind=jnp.bfloat16):
    entries = jax.random.normal(own_key, extent, jnp.float32) * scale
    return jnp.minimum(jnp.maximum(entries, -reach), reach).astype(kind)


def setup_inputs(seed: int = 0) -> dict:
    keys = jax.random.split(jax.random.key(seed), 7)
    return {
        "history": draw_history(jax.random.fold_in(keys[6], 71), 0),
        "event_cat": draw_event_cat(jax.random.fold_in(keys[6], 71), 0),
        "candidates": draw_candidates(jax.random.fold_in(keys[6], 71), 0),
        "cand_cat": draw_cand_cat(jax.random.fold_in(keys[6], 71), 0),
        "w_input": scatter_about(keys[4], (2 * D, HID), (2 * D) ** -0.5, 0.375),
        "w_output": scatter_about(keys[5], (HID, D), HID ** -0.5, 0.25),
    }


def attend(queries, slots, usable):
    group = queries.shape[0]
    count = queries.shape[1]
    width = queries.shape[2]
    head_size = width // HEADS
    query_heads = queries.astype(jnp.float32).reshape(group, count, HEADS, head_size)
    key_heads = slots.astype(jnp.float32).reshape(group, -1, HEADS, head_size)
    scores = jnp.einsum("gchk,gshk->ghcs", query_heads, key_heads) * (head_size ** -0.5)
    scores = jnp.where(usable[:, None, None, :], scores, -1e30)
    row_max = jnp.max(scores, axis=-1, keepdims=True)
    expo = jnp.exp(scores - row_max)
    total = jnp.sum(expo, axis=-1, keepdims=True)
    weights = (expo / total).astype(jnp.bfloat16)
    interest = jnp.einsum("ghcs,gshk->gchk", weights.astype(jnp.float32), key_heads)
    return interest.reshape(group, count, width).astype(jnp.bfloat16)


def user_group(history, event_cat, candidates, cand_cat, w_input, w_output):
    group = history.shape[0]
    blocks = EVENTS // E_DEV
    hits = jnp.any(event_cat[:, :, None] == cand_cat[:, None, :], axis=-1).reshape(group, blocks, E_DEV)
    slot_rank = jnp.cumsum(hits.astype(jnp.int32), axis=-1) - 1
    places = jnp.arange(CAP, dtype=jnp.int32)
    selector = (hits[:, :, None, :] & (slot_rank[:, :, None, :] == places[None, None, :, None])).astype(jnp.float32)
    events = history.reshape(group, blocks, E_DEV, D).astype(jnp.float32)
    slots = jnp.einsum("gbse,gbed->gbsd", selector, events).astype(jnp.bfloat16).reshape(group, blocks * CAP, D)
    counts = jnp.sum(hits.astype(jnp.int32), axis=-1)
    usable = (places[None, None, :] < counts[:, :, None]).reshape(group, blocks * CAP)
    interest = attend(candidates, slots, usable)
    rows = group * CANDS
    hidden = jnp.dot(candidates.reshape(rows, D), w_input[:D], preferred_element_type=jnp.float32)
    hidden = hidden + jnp.dot(interest.reshape(rows, D), w_input[D:], preferred_element_type=jnp.float32)
    hidden = jax.nn.silu(hidden).astype(jnp.bfloat16)
    result = jnp.dot(hidden, w_output, preferred_element_type=jnp.float32).astype(jnp.bfloat16)
    return result.reshape(group, CANDS, D)


def reference(history, event_cat, candidates, cand_cat, w_input, w_output):
    group = math.gcd(USERS, 16)
    packs = USERS // group

    def one_pack(pieces):
        return user_group(pieces[0], pieces[1], pieces[2], pieces[3], w_input, w_output)

    result = lax.map(one_pack, (history.reshape(packs, group, EVENTS, D), event_cat.reshape(packs, group, EVENTS), candidates.reshape(packs, group, CANDS, D), cand_cat.reshape(packs, group, CANDS)))
    return result.reshape(USERS, CANDS, D)
```

```python
import functools
import jax
import jax.numpy as jnp
from jax import lax
from jax.experimental import pallas as pl
from jax.experimental.pallas import tpu as pltpu
from jax.sharding import PartitionSpec as P

AXES = ("role", "shard")
MESH = pl.DeviceIdType.MESH
DEVS = 128
SIDE = 4
E_DEV = 20
QCAT = 8
CAP = 8
OWN = 8
PAIRS = OWN // 2
LANES = E_DEV * OWN
WIDTH = 128


def partner(i, role, y, z, x):
    r = lax.rem(role + lax.rem(i, 2), 2)
    j = i // 2
    px = lax.rem(x + lax.rem(j, 4), 4)
    pz = lax.rem(z + lax.rem(j // 4, 4), 4)
    py = lax.rem(y + j // 16, 4)
    return r, py * 16 + pz * 4 + px


def exchange_kernel(hist_hbm, cats_ref, cand_cat_ref, recv_ref, cnt_in_ref,
                    hist_ref, id_row_ref, ids_ref, key_ref, cnt_ref, send_ref,
                    hist_sems, id_send, id_recv, cnt_send, cnt_recv, data_send, data_recv):
    role = lax.axis_index("role")
    shard = lax.axis_index("shard")
    y, z, x = shard // 16, lax.rem(shard // 4, 4), lax.rem(shard, 4)
    me = role * 64 + shard

    barrier = pltpu.get_barrier_semaphore()

    def greet(i, carry):
        r, s = partner(i, role, y, z, x)
        pl.semaphore_signal(barrier, inc=1, device_id={"role": r, "shard": s}, device_id_type=MESH)
        return carry

    lax.fori_loop(1, DEVS, greet, 0)

    loads = [
        pltpu.make_async_copy(hist_hbm.at[e], hist_ref.at[:, pl.ds(e * OWN, OWN), :], hist_sems.at[e])
        for e in range(E_DEV)
    ]
    for load in loads:
        load.start()

    cats = cand_cat_ref[...].astype(jnp.float32)
    lane = lax.broadcasted_iota(jnp.int32, (OWN, WIDTH), 1)
    sub = lax.broadcasted_iota(jnp.int32, (OWN, WIDTH), 0)
    spread = jnp.zeros((OWN, WIDTH), jnp.float32)
    last = jnp.full((OWN, 1), -1.0, jnp.float32)
    for k in range(QCAT):
        last = jnp.min(jnp.where(cats > last, cats, 4096.0), axis=1, keepdims=True)
        spot = (lax.rem(lane, 8) == sub) & (lax.rem(lane // 8, 8) == k)
        spread = jnp.where(spot, last, spread)
    row = jnp.sum(spread, axis=0, keepdims=True).astype(jnp.int32)
    low = lax.rem(row, 32)
    lane1 = lax.broadcasted_iota(jnp.int32, (1, WIDTH), 1)
    id_row_ref[...] = jnp.where(lane1 < 64, row - low, low).astype(jnp.float32)

    pl.semaphore_wait(barrier, DEVS - 1)

    def send_ids(i, carry):
        r, s = partner(i, role, y, z, x)
        pltpu.make_async_remote_copy(
            src_ref=id_row_ref, dst_ref=ids_ref.at[pl.ds(me, 1)],
            send_sem=id_send, recv_sem=id_recv,
            device_id={"role": r, "shard": s}, device_id_type=MESH).start()
        return carry

    lax.fori_loop(1, DEVS, send_ids, 0)
    pltpu.make_async_copy(id_row_ref, ids_ref.at[pl.ds(me, 1)], id_recv).start()
    pltpu.make_async_copy(ids_ref, ids_ref, id_recv).wait()

    ids = ids_ref[...].astype(jnp.bfloat16)
    lane_i = lax.broadcasted_iota(jnp.int32, (DEVS, WIDTH), 1)
    stacked = jnp.concatenate(
        [jnp.where(lax.rem(lane_i // 8, 8) == k, ids, jnp.zeros_like(ids)) for k in range(QCAT)], axis=0)
    er = lax.broadcasted_iota(jnp.int32, (WIDTH, LANES), 0)
    ec = lax.broadcasted_iota(jnp.int32, (WIDTH, LANES), 1)
    expand = jnp.where(lax.rem(er, 8) == lax.rem(ec, 8), 1.0, 0.0).astype(jnp.bfloat16)
    wanted = jnp.dot(stacked, expand, preferred_element_type=jnp.float32)
    events = cats_ref[...]
    hit = events == wanted[0:DEVS]
    for k in range(1, QCAT):
        hit = hit | (events == wanted[k * DEVS:(k + 1) * DEVS])
    hits = jnp.where(hit, 1.0, 0.0).astype(jnp.bfloat16)
    a = lax.broadcasted_iota(jnp.int32, (LANES, LANES), 0)
    b = lax.broadcasted_iota(jnp.int32, (LANES, LANES), 1)
    ua, ub = lax.rem(a, 8), lax.rem(b, 8)
    before = ((ua == ub) & (a < b)) | ((ua + 1 == ub) & (lax.rem(ub, 2) == 1))
    rank = jnp.dot(hits, jnp.where(before, 1.0, 0.0).astype(jnp.bfloat16), preferred_element_type=jnp.float32)
    lane_k = lax.broadcasted_iota(jnp.int32, (DEVS, LANES), 1)
    base = (lax.rem(lane_k, 8) // 2 * CAP).astype(jnp.float32)
    key_ref[...] = jnp.where(hit, base + rank, -1.0)
    ca = lax.broadcasted_iota(jnp.int32, (LANES, WIDTH), 0)
    cb = lax.broadcasted_iota(jnp.int32, (LANES, WIDTH), 1)
    lead_of = jnp.where(lax.rem(ca, 8) == cb // 8 * 2, 1.0, 0.0).astype(jnp.bfloat16)
    cnt_ref[...] = jnp.dot(hits, lead_of, preferred_element_type=jnp.float32)

    for load in loads:
        load.wait()

    rows = lax.broadcasted_iota(jnp.int32, (PAIRS * CAP, LANES), 0).astype(jnp.float32)

    def fill(i):
        r, s = partner(i, role, y, z, x)
        t = r * 64 + s
        pick = jnp.where(key_ref[pl.ds(t, 1), :] == rows, 1.0, 0.0).astype(jnp.bfloat16)
        packed = jnp.dot(pick, hist_ref[t], preferred_element_type=jnp.float32)
        send_ref[i] = packed.astype(jnp.bfloat16).reshape(PAIRS, CAP, WIDTH)
        return r, s, t

    def data_step(i, carry):
        r, s, t = fill(i)
        pltpu.make_async_remote_copy(
            src_ref=cnt_ref.at[pl.ds(t, 1)], dst_ref=cnt_in_ref.at[pl.ds(me, 1)],
            send_sem=cnt_send, recv_sem=cnt_recv,
            device_id={"role": r, "shard": s}, device_id_type=MESH).start()
        pltpu.make_async_remote_copy(
            src_ref=send_ref.at[i], dst_ref=recv_ref.at[:, me],
            send_sem=data_send, recv_sem=data_recv,
            device_id={"role": r, "shard": s}, device_id_type=MESH).start()
        return carry

    lax.fori_loop(1, DEVS, data_step, 0)
    fill(0)
    pltpu.make_async_copy(send_ref.at[0], recv_ref.at[:, me], data_recv).start()
    pltpu.make_async_copy(cnt_ref.at[pl.ds(me, 1)], cnt_in_ref.at[pl.ds(me, 1)], cnt_recv).start()
    pltpu.make_async_copy(recv_ref, recv_ref, data_recv).wait()
    pltpu.make_async_copy(cnt_in_ref, cnt_in_ref, cnt_recv).wait()
    others = pl.ds(0, DEVS - 1)
    pltpu.make_async_copy(send_ref.at[others], send_ref.at[others], data_send).wait()
    pltpu.make_async_copy(cnt_ref.at[others], cnt_ref.at[others], cnt_send).wait()
    pltpu.make_async_copy(ids_ref.at[others], ids_ref.at[others], id_send).wait()


def exchange(history, event_cat, cand_cat):
    hist = history.transpose(1, 0, 2).reshape(E_DEV, DEVS, OWN, WIDTH)
    cats = event_cat.astype(jnp.float32).T.reshape(E_DEV, DEVS, OWN).transpose(1, 0, 2).reshape(DEVS, LANES)
    vm = pl.BlockSpec(memory_space=pltpu.VMEM)
    return pl.pallas_call(
        exchange_kernel,
        out_shape=(jax.ShapeDtypeStruct((PAIRS, DEVS, CAP, WIDTH), jnp.bfloat16),
                   jax.ShapeDtypeStruct((DEVS, WIDTH), jnp.float32)),
        in_specs=[pl.BlockSpec(memory_space=pl.ANY), vm, vm],
        out_specs=(vm, vm),
        scratch_shapes=[
            pltpu.VMEM((DEVS, LANES, WIDTH), jnp.bfloat16),
            pltpu.VMEM((1, WIDTH), jnp.float32),
            pltpu.VMEM((DEVS, WIDTH), jnp.float32),
            pltpu.VMEM((DEVS, LANES), jnp.float32),
            pltpu.VMEM((DEVS, WIDTH), jnp.float32),
            pltpu.VMEM((DEVS, PAIRS, CAP, WIDTH), jnp.bfloat16),
            pltpu.SemaphoreType.DMA((E_DEV,)),
        ] + [pltpu.SemaphoreType.DMA] * 6,
        compiler_params=pltpu.CompilerParams(collective_id=0, has_side_effects=True,
                                             vmem_limit_bytes=60 << 20),
        name="exchange",
    )(hist, cats, cand_cat)


def head_attention(history_slots, lead, candidates, w_input, w_output):
    own = candidates.shape[0]
    slots = history_slots.reshape(PAIRS, DEVS * CAP, WIDTH)
    counts = lead[:, :PAIRS * CAP].T.reshape(PAIRS, CAP, DEVS).transpose(0, 2, 1)
    is_lead = (jnp.arange(CAP, dtype=jnp.float32)[None, None, :] < counts).reshape(PAIRS, DEVS * CAP)
    usable = jnp.stack([is_lead, ~is_lead], axis=1).reshape(own, DEVS * CAP)
    keys = jnp.repeat(slots, 2, axis=0).reshape(own, DEVS * CAP, 4, 32)
    q = candidates.reshape(own, -1, 4, 32)
    s = jnp.einsum("gchk,gshk->ghcs", q, keys, preferred_element_type=jnp.float32) * 32 ** -0.5
    s = jnp.where(usable[:, None, None, :], s, -1e30)
    e = jnp.exp(s - jnp.max(s, axis=-1, keepdims=True))
    w = (e / jnp.sum(e, axis=-1, keepdims=True)).astype(jnp.bfloat16)
    interest = jnp.einsum("ghcs,gshk->gchk", w, keys, preferred_element_type=jnp.float32)
    interest = interest.reshape(own, -1, WIDTH).astype(jnp.bfloat16)
    rows = jnp.concatenate([candidates, interest], axis=-1)
    hidden = jax.nn.silu(jnp.einsum("gck,kn->gcn", rows, w_input, preferred_element_type=jnp.float32)).astype(jnp.bfloat16)
    return jnp.einsum("gcn,nd->gcd", hidden, w_output, preferred_element_type=jnp.float32).astype(jnp.bfloat16)


def local(history, event_cat, candidates, cand_cat, w_input, w_output):
    slots, lead = exchange(history, event_cat, cand_cat)
    return head_attention(slots, lead, candidates, w_input, w_output)


def solution(mesh):
    return jax.shard_map(
        local, mesh=mesh,
        in_specs=(P(None, AXES, None), P(None, AXES), P(AXES, None, None), P(AXES, None), P(), P()),
        out_specs=P(AXES, None, None), check_vma=False)
```

```python
import math

import jax
import jax.numpy as jnp
from jax import lax
from jax.experimental import pallas as pl
from jax.experimental.pallas import tpu as pltpu
from jax.sharding import PartitionSpec as P

AXES = ("role", "shard")
MESH = pl.DeviceIdType.MESH
DEVS = 128
SIDE = 4
E_DEV = 20
QCAT = 8
CAP = 8
OWN = 8
PAIRS = OWN // 2
LANES = E_DEV * OWN
WIDTH = 128


CANDS = 200
ROWS = 208
HEADS = 4
CHUNKS = 4
PER_CHUNK = DEVS // CHUNKS
SLOTS = PER_CHUNK * CAP
BLOCK = 16
SCALE = 32 ** -0.5 * math.log2(math.e)
FAR = (2, 3, 1, 0)


def far(k):
    late = k // 2
    return (2 + k) * (1 - late) + (3 - k) * late


def place():
    role = lax.axis_index("role")
    shard = lax.axis_index("shard")
    return role, shard // 16, lax.rem(shard // 4, 4), lax.rem(shard, 4)


def partner(block, k, at):
    role, y, z, x = at
    r = lax.rem(role + 1 - k % 2, 2)
    px = lax.rem(x + FAR[(k // 2) % 4], 4)
    pz = lax.rem(z + far(lax.rem(block, 2) * 2 + k // 8), 4)
    py = lax.rem(y + far(block // 2), 4)
    return r, py * 16 + pz * 4 + px


def signal(sem, r, s):
    pl.semaphore_signal(sem, inc=1, device_id={"role": r, "shard": s}, device_id_type=MESH)


def push(src, dst, send_sem, recv_sem, r, s):
    pltpu.make_async_remote_copy(
        src_ref=src, dst_ref=dst, send_sem=send_sem, recv_sem=recv_sem,
        device_id={"role": r, "shard": s}, device_id_type=MESH).start()


def landed(ref, sem):
    pltpu.make_async_copy(ref, ref, sem).wait()


def line_peers(at):
    role, y, z, x = at
    return [(lax.rem(role + dr, 2), y * 16 + z * 4 + lax.rem(x + dx, 4))
            for dr in range(2) for dx in range(4) if dr or dx]


def plane_peers(at):
    role, y, z, x = at
    return [(role, lax.rem(y + dy, 4) * 16 + lax.rem(z + dz, 4) * 4 + x)
            for dy in FAR for dz in FAR if dy or dz]


def distinct_row(cats):
    lane = lax.broadcasted_iota(jnp.int32, (OWN, WIDTH), 1)
    sub = lax.broadcasted_iota(jnp.int32, (OWN, WIDTH), 0)
    spread = jnp.zeros((OWN, WIDTH), jnp.float32)
    last = jnp.full((OWN, 1), -1.0, jnp.float32)
    for k in range(QCAT):
        last = jnp.min(jnp.where(cats > last, cats, 4096.0), axis=1, keepdims=True)
        spot = (lax.rem(lane, 8) == sub) & (lax.rem(lane // 8, 8) == k)
        spread = jnp.where(spot, last, spread)
    row = jnp.sum(spread, axis=0, keepdims=True).astype(jnp.int32)
    low = lax.rem(row, 32)
    lane1 = lax.broadcasted_iota(jnp.int32, (1, WIDTH), 1)
    return jnp.where(lane1 < 64, row - low, low).astype(jnp.float32)


def matched(ids, events):
    ids = ids.astype(jnp.bfloat16)
    lane_i = lax.broadcasted_iota(jnp.int32, (DEVS, WIDTH), 1)
    er = lax.broadcasted_iota(jnp.int32, (WIDTH, LANES), 0)
    ec = lax.broadcasted_iota(jnp.int32, (WIDTH, LANES), 1)
    expand = jnp.where(lax.rem(er, 8) == lax.rem(ec, 8), 1.0, 0.0).astype(jnp.bfloat16)
    hit = None
    for k in range(QCAT):
        only = jnp.where(lax.rem(lane_i // 8, 8) == k, ids, jnp.zeros_like(ids))
        same = events == jnp.dot(only, expand, preferred_element_type=jnp.float32)
        hit = same if hit is None else hit | same
    hits = jnp.where(hit, 1.0, 0.0).astype(jnp.bfloat16)
    a = lax.broadcasted_iota(jnp.int32, (LANES, LANES), 0)
    b = lax.broadcasted_iota(jnp.int32, (LANES, LANES), 1)
    ua, ub = lax.rem(a, 8), lax.rem(b, 8)
    before = ((ua == ub) & (a < b)) | ((ua + 1 == ub) & (lax.rem(ub, 2) == 1))
    rank = jnp.dot(hits, jnp.where(before, 1.0, 0.0).astype(jnp.bfloat16), preferred_element_type=jnp.float32)
    lane_k = lax.broadcasted_iota(jnp.int32, (DEVS, LANES), 1)
    base = (lax.rem(lane_k, 8) // 2 * CAP).astype(jnp.float32)
    ca = lax.broadcasted_iota(jnp.int32, (LANES, WIDTH), 0)
    cb = lax.broadcasted_iota(jnp.int32, (LANES, WIDTH), 1)
    lead_of = jnp.where(lax.rem(ca, 8) == cb // 32 * 2, 1.0, 0.0).astype(jnp.bfloat16)
    lead = jnp.dot(hits, lead_of, preferred_element_type=jnp.float32)
    return jnp.where(hit, base + rank, -1.0), lead


def fill_queries(cand_ref, q_ref):
    lane = lax.broadcasted_iota(jnp.int32, (CANDS, WIDTH), 1)
    pick = lax.broadcasted_iota(jnp.int32, (ROWS, WIDTH), 1)

    def one(u, carry):
        cand = cand_ref[u]
        column = u // 2 * 32 + lax.rem(u, 2)
        bias = jnp.where(pick == column, 1.0, 0.0).astype(jnp.bfloat16)
        for h in range(HEADS):
            q_ref[u, h, CANDS:ROWS, 0:WIDTH] = jnp.zeros((ROWS - CANDS, WIDTH), jnp.bfloat16)
            q_ref[u, h, 0:CANDS, 0:WIDTH] = jnp.where(lane // 32 == h, cand, jnp.zeros_like(cand))
            q_ref[u, h, :, WIDTH:] = bias
        return carry

    lax.fori_loop(0, OWN, one, 0)


def bias_columns(lead):
    r = lax.broadcasted_iota(jnp.int32, (SLOTS, PER_CHUNK), 0)
    b = lax.broadcasted_iota(jnp.int32, (SLOTS, PER_CHUNK), 1)
    repeat = jnp.where(r // CAP == b, 1.0, 0.0).astype(jnp.bfloat16)
    lead = jnp.dot(repeat, lead.astype(jnp.bfloat16), preferred_element_type=jnp.float32)
    slot = lax.rem(lax.broadcasted_iota(jnp.int32, (SLOTS, WIDTH), 0), CAP).astype(jnp.float32)
    follow = lax.rem(lax.broadcasted_iota(jnp.int32, (SLOTS, WIDTH), 1), 2)
    mine = jnp.where(follow == 1, slot - lead, lead - slot - 1.0) >= 0.0
    return jnp.where(mine, 0.0, -1e30).astype(jnp.bfloat16)


def pair_step(p, keys, bias, q_ref, m_ref, num_ref, den_ref):
    lane = lax.broadcasted_iota(jnp.int32, (SLOTS, WIDTH), 1)
    out_lane = lax.broadcasted_iota(jnp.int32, (ROWS, WIDTH), 1)
    key_ext = jnp.concatenate([keys, bias], axis=1)
    values = []
    for h in range(HEADS):
        own = lane // 32 == h
        ones = jnp.where(own, 1.0, 0.0).astype(jnp.bfloat16)
        values.append(jnp.concatenate([jnp.where(own, keys, jnp.zeros_like(keys)), ones], axis=1))
    for v in range(2):
        u = p * 2 + v
        total = None
        alpha = None
        for h in range(HEADS):
            s = lax.dot_general(q_ref[u, h], key_ext, (((1,), (1,)), ((), ())),
                                preferred_element_type=jnp.float32) * SCALE
            old = m_ref[u, h]
            new = jnp.maximum(old, jnp.max(s, axis=1, keepdims=True))
            m_ref[u, h] = new
            weights = jnp.exp2(s - jnp.concatenate([new, new], axis=1)).astype(jnp.bfloat16)
            part = jnp.dot(weights, values[h], preferred_element_type=jnp.float32)
            total = part if total is None else total + part
            shrink = jnp.exp2(old - new)
            alpha = shrink if alpha is None else jnp.where(out_lane // 32 == h, shrink, alpha)
        num_ref[u] = num_ref[u] * alpha + total[:, :WIDTH]
        den_ref[u] = den_ref[u] * alpha + total[:, WIDTH:]


def fused_kernel(hist_hbm, cats_ref, cand_cat_ref, cand_ref, out_ref,
                 hist_ref, id_row_ref, ids_ref, key_ref, cnt_ref, send_ref, cnt_in_ref, recv_ref,
                 q_ref, m_ref, num_ref, den_ref, bias_ref,
                 hist_sems, line_send, line_recv, plane_send, plane_recv,
                 cnt_send, cnt_recv, data_send, data_recv):
    at = place()
    role, y, z, x = at
    base = y * 16 + z * 4
    me = role * 64 + base + x
    line, plane = line_peers(at), plane_peers(at)

    barrier = pltpu.get_barrier_semaphore()
    for r, s in plane + line:
        signal(barrier, r, s)
    loads = [
        pltpu.make_async_copy(hist_hbm.at[e], hist_ref.at[:, pl.ds(e * OWN, OWN), :], hist_sems.at[e])
        for e in range(E_DEV)
    ]
    for load in loads:
        load.start()
    id_row_ref[...] = distinct_row(cand_cat_ref[...].astype(jnp.float32))
    pl.semaphore_wait(barrier, len(line) + len(plane))

    for r, s in line:
        push(id_row_ref, ids_ref.at[pl.ds(me, 1)], line_send, line_recv, r, s)
    pltpu.make_async_copy(id_row_ref, ids_ref.at[pl.ds(me, 1)], line_recv).start()
    fill_queries(cand_ref, q_ref)
    landed(ids_ref.at[pl.ds(0, 8)], line_recv)
    for r, s in plane:
        for half in range(2):
            rows = ids_ref.at[pl.ds(half * 64 + base, 4)]
            push(rows, rows, plane_send, plane_recv, r, s)
    m_ref[...] = jnp.full_like(m_ref, -3e38)
    num_ref[...] = jnp.zeros_like(num_ref)
    den_ref[...] = jnp.zeros_like(den_ref)
    landed(ids_ref.at[pl.ds(0, 120)], plane_recv)

    key_ref[...], cnt_ref[...] = matched(ids_ref[...], cats_ref[...])
    for load in loads:
        load.wait()
    rows = lax.broadcasted_iota(jnp.int32, (PAIRS * CAP, LANES), 0).astype(jnp.float32)

    def data_step(block, carry):
        peers = [partner(block, k, at) for k in range(BLOCK)]
        first = block * BLOCK
        chunk = block // (PER_CHUNK // BLOCK)
        for k, (r, s) in enumerate(peers):
            t = r * 64 + s
            pick = jnp.where(key_ref[pl.ds(t, 1), :] == rows, 1.0, 0.0).astype(jnp.bfloat16)
            packed = jnp.dot(pick, hist_ref[t], preferred_element_type=jnp.float32)
            send_ref[first + k] = packed.astype(jnp.bfloat16).reshape(PAIRS, CAP, WIDTH)
        for k, (r, s) in enumerate(peers):
            i = first + k
            cnt_src, cnt_dst = cnt_ref.at[pl.ds(r * 64 + s, 1)], cnt_in_ref.at[pl.ds(i, 1)]
            src, dst = send_ref.at[i], recv_ref.at[:, pl.ds(pl.multiple_of(i * CAP, CAP), CAP), :]

            def away(r=r, s=s, cnt_src=cnt_src, cnt_dst=cnt_dst, src=src, dst=dst):
                push(cnt_src, cnt_dst, cnt_send, cnt_recv.at[chunk], r, s)
                push(src, dst, data_send, data_recv.at[chunk], r, s)

            if k < BLOCK - 1:
                away()
            else:
                last = block == DEVS // BLOCK - 1
                pl.when(jnp.logical_not(last))(away)

                @pl.when(last)
                def _(cnt_src=cnt_src, cnt_dst=cnt_dst, src=src, dst=dst):
                    pltpu.make_async_copy(cnt_src, cnt_dst, cnt_recv.at[chunk]).start()
                    pltpu.make_async_copy(src, dst, data_recv.at[chunk]).start()
        return carry

    lax.fori_loop(0, DEVS // BLOCK, data_step, 0)

    def chunk_step(c, carry):
        counts = cnt_in_ref.at[pl.ds(c * PER_CHUNK, PER_CHUNK)]
        landed(counts, cnt_recv.at[c])
        slots = pl.ds(pl.multiple_of(c * SLOTS, SLOTS), SLOTS)
        landed(recv_ref.at[:, slots, :], data_recv.at[c])
        bias_ref[...] = bias_columns(counts[...])

        def one(p, carry):
            pair_step(p, recv_ref[p, slots, :], bias_ref[...], q_ref, m_ref, num_ref, den_ref)
            return carry

        return lax.fori_loop(0, PAIRS, one, carry)

    lax.fori_loop(0, CHUNKS, chunk_step, 0)

    def finish(u, carry):
        out_ref[u] = (num_ref[u, 0:CANDS, :] / den_ref[u, 0:CANDS, :]).astype(jnp.bfloat16)
        return carry

    lax.fori_loop(0, OWN, finish, 0)

    others = pl.ds(0, DEVS - 1)
    landed(send_ref.at[others], data_send)
    landed(cnt_ref.at[others], cnt_send)
    landed(ids_ref.at[pl.ds(0, 7)], line_send)
    landed(ids_ref.at[pl.ds(0, 120)], plane_send)


def interest_of(history, event_cat, candidates, cand_cat):
    hist = history.transpose(1, 0, 2).reshape(E_DEV, DEVS, OWN, WIDTH)
    cats = event_cat.astype(jnp.float32).T.reshape(E_DEV, DEVS, OWN).transpose(1, 0, 2).reshape(DEVS, LANES)
    vm = pl.BlockSpec(memory_space=pltpu.VMEM)
    f32, bf16 = jnp.float32, jnp.bfloat16
    return pl.pallas_call(
        fused_kernel,
        out_shape=jax.ShapeDtypeStruct((OWN, CANDS, WIDTH), bf16),
        in_specs=[pl.BlockSpec(memory_space=pl.ANY), vm, vm, vm],
        out_specs=vm,
        scratch_shapes=[
            pltpu.VMEM((DEVS, LANES, WIDTH), bf16),
            pltpu.VMEM((1, WIDTH), f32),
            pltpu.VMEM((DEVS, WIDTH), f32),
            pltpu.VMEM((DEVS, LANES), f32),
            pltpu.VMEM((DEVS, WIDTH), f32),
            pltpu.VMEM((DEVS, PAIRS, CAP, WIDTH), bf16),
            pltpu.VMEM((DEVS, WIDTH), f32),
            pltpu.VMEM((PAIRS, DEVS * CAP, WIDTH), bf16),
            pltpu.VMEM((OWN, HEADS, ROWS, 2 * WIDTH), bf16),
            pltpu.VMEM((OWN, HEADS, ROWS, WIDTH), f32),
            pltpu.VMEM((OWN, ROWS, WIDTH), f32),
            pltpu.VMEM((OWN, ROWS, WIDTH), f32),
            pltpu.VMEM((SLOTS, WIDTH), bf16),
            pltpu.SemaphoreType.DMA((E_DEV,)),
            pltpu.SemaphoreType.DMA, pltpu.SemaphoreType.DMA, pltpu.SemaphoreType.DMA, pltpu.SemaphoreType.DMA,
            pltpu.SemaphoreType.DMA, pltpu.SemaphoreType.DMA((CHUNKS,)),
            pltpu.SemaphoreType.DMA, pltpu.SemaphoreType.DMA((CHUNKS,)),
        ],
        compiler_params=pltpu.CompilerParams(collective_id=0, has_side_effects=True,
                                             vmem_limit_bytes=56 << 20),
        name="match_and_attend",
    )(hist, cats, cand_cat, candidates)


def local(history, event_cat, candidates, cand_cat, w_input, w_output):
    interest = interest_of(history, event_cat, candidates, cand_cat)
    rows = OWN * CANDS
    hidden = jnp.dot(candidates.reshape(rows, WIDTH), w_input[:WIDTH], preferred_element_type=jnp.float32)
    hidden += jnp.dot(interest.reshape(rows, WIDTH), w_input[WIDTH:], preferred_element_type=jnp.float32)
    hidden = jax.nn.silu(hidden).astype(jnp.bfloat16)
    result = jnp.dot(hidden, w_output, preferred_element_type=jnp.float32).astype(jnp.bfloat16)
    return result.reshape(OWN, CANDS, WIDTH)


def solution(mesh):
    return jax.shard_map(
        local, mesh=mesh,
        in_specs=(P(None, AXES, None), P(None, AXES), P(AXES, None, None), P(AXES, None), P(), P()),
        out_specs=P(AXES, None, None), check_vma=False)
```

```python
import math

import jax
import jax.numpy as jnp
from jax import lax
from jax.experimental import pallas as pl
from jax.experimental.pallas import tpu as pltpu
from jax.sharding import PartitionSpec as P

AXES = ("role", "shard")
MESH = pl.DeviceIdType.MESH
DEVS = 128
SIDE = 4
E_DEV = 20
QCAT = 8
CAP = 8
OWN = 8
PAIRS = OWN // 2
LANES = E_DEV * OWN
WIDTH = 128


CANDS = 200
ROWS = 208
HEADS = 4
HID = 512
CHUNKS = 4
PER_CHUNK = DEVS // CHUNKS
SLOTS = PER_CHUNK * CAP
BLOCK = 16
SCALE = 32 ** -0.5 * math.log2(math.e)
FAR = (2, 3, 1, 0)


def place():
    role = lax.axis_index("role")
    shard = lax.axis_index("shard")
    return role, shard // 16, lax.rem(shard // 4, 4), lax.rem(shard, 4)


def partner(block, k, at):
    role, y, z, x = at
    r = lax.rem(role + 1 - lax.rem(block, 2), 2)
    dy, dz = FAR[k // 4], FAR[k % 4]
    px = lax.rem(x + block // 2 + 1 + 8 - dy - dz, 4)
    return r, lax.rem(y + dy, 4) * 16 + lax.rem(z + dz, 4) * 4 + px


def signal(sem, r, s):
    pl.semaphore_signal(sem, inc=1, device_id={"role": r, "shard": s}, device_id_type=MESH)


def push(src, dst, send_sem, recv_sem, r, s):
    pltpu.make_async_remote_copy(
        src_ref=src, dst_ref=dst, send_sem=send_sem, recv_sem=recv_sem,
        device_id={"role": r, "shard": s}, device_id_type=MESH).start()


def landed(ref, sem):
    pltpu.make_async_copy(ref, ref, sem).wait()


def line_peers(at):
    role, y, z, x = at
    return [(lax.rem(role + dr, 2), y * 16 + z * 4 + lax.rem(x + dx, 4))
            for dr in range(2) for dx in range(4) if dr or dx]


def plane_peers(at):
    role, y, z, x = at
    return [(role, lax.rem(y + dy, 4) * 16 + lax.rem(z + dz, 4) * 4 + x)
            for dy in FAR for dz in FAR if dy or dz]


def distinct_row(cats):
    lane = lax.broadcasted_iota(jnp.int32, (OWN, WIDTH), 1)
    sub = lax.broadcasted_iota(jnp.int32, (OWN, WIDTH), 0)
    spread = jnp.zeros((OWN, WIDTH), jnp.float32)
    last = jnp.full((OWN, 1), -1.0, jnp.float32)
    for k in range(QCAT):
        last = jnp.min(jnp.where(cats > last, cats, 4096.0), axis=1, keepdims=True)
        spot = (lax.rem(lane, 8) == sub) & (lax.rem(lane // 8, 8) == k)
        spread = jnp.where(spot, last, spread)
    row = jnp.sum(spread, axis=0, keepdims=True).astype(jnp.int32)
    low = lax.rem(row, 32)
    lane1 = lax.broadcasted_iota(jnp.int32, (1, WIDTH), 1)
    return jnp.where(lane1 < 64, row - low, low).astype(jnp.float32)


def flat_events(cats_ref, pad_ref, cols_ref):
    pad_ref[...] = jnp.zeros_like(pad_ref)
    pad_ref[0:E_DEV, :] = cats_ref[...]
    for j in range(OWN):
        cols_ref[j * WIDTH:(j + 1) * WIDTH, 0:32] = pad_ref[:, j * WIDTH:(j + 1) * WIDTH].T
    e = lax.broadcasted_iota(jnp.int32, (32, LANES), 0)
    lane = lax.broadcasted_iota(jnp.int32, (32, LANES), 1)
    flat = None
    for u in range(OWN):
        value = cols_ref[pl.ds(u, DEVS, stride=OWN), 0:32]
        low = lax.rem(value, 32)
        spot = jnp.where(lane == e * OWN + u, 1.0, 0.0).astype(jnp.bfloat16)
        for part in (value - low, low):
            moved = jnp.dot(part.astype(jnp.float32).astype(jnp.bfloat16), spot, preferred_element_type=jnp.float32)
            flat = moved if flat is None else flat + moved
    return flat


def matched(ids, events):
    ids = ids.astype(jnp.bfloat16)
    lane_i = lax.broadcasted_iota(jnp.int32, (DEVS, WIDTH), 1)
    er = lax.broadcasted_iota(jnp.int32, (WIDTH, LANES), 0)
    ec = lax.broadcasted_iota(jnp.int32, (WIDTH, LANES), 1)
    expand = jnp.where(lax.rem(er, 8) == lax.rem(ec, 8), 1.0, 0.0).astype(jnp.bfloat16)
    hit = None
    for k in range(QCAT):
        only = jnp.where(lax.rem(lane_i // 8, 8) == k, ids, jnp.zeros_like(ids))
        same = events == jnp.dot(only, expand, preferred_element_type=jnp.float32)
        hit = same if hit is None else hit | same
    hits = jnp.where(hit, 1.0, 0.0).astype(jnp.bfloat16)
    a = lax.broadcasted_iota(jnp.int32, (LANES, LANES), 0)
    b = lax.broadcasted_iota(jnp.int32, (LANES, LANES), 1)
    ua, ub = lax.rem(a, 8), lax.rem(b, 8)
    before = ((ua == ub) & (a < b)) | ((ua + 1 == ub) & (lax.rem(ub, 2) == 1))
    rank = jnp.dot(hits, jnp.where(before, 1.0, 0.0).astype(jnp.bfloat16), preferred_element_type=jnp.float32)
    lane_k = lax.broadcasted_iota(jnp.int32, (DEVS, LANES), 1)
    base = (lax.rem(lane_k, 8) // 2 * CAP).astype(jnp.float32)
    ca = lax.broadcasted_iota(jnp.int32, (LANES, WIDTH), 0)
    cb = lax.broadcasted_iota(jnp.int32, (LANES, WIDTH), 1)
    lead_of = jnp.where(lax.rem(ca, 8) == cb // 32 * 2, 1.0, 0.0).astype(jnp.bfloat16)
    lead = jnp.dot(hits, lead_of, preferred_element_type=jnp.float32)
    return jnp.where(hit, base + rank, -1.0), lead


def fill_queries(cand_ref, q_ref):
    lane = lax.broadcasted_iota(jnp.int32, (CANDS, WIDTH), 1)
    pick = lax.broadcasted_iota(jnp.int32, (ROWS, WIDTH), 1)

    def one(u, carry):
        cand = cand_ref[u]
        column = u // 2 * 32 + lax.rem(u, 2)
        bias = jnp.where(pick == column, 1.0, 0.0).astype(jnp.bfloat16)
        for h in range(HEADS):
            q_ref[u, h, CANDS:ROWS, 0:WIDTH] = jnp.zeros((ROWS - CANDS, WIDTH), jnp.bfloat16)
            q_ref[u, h, 0:CANDS, 0:WIDTH] = jnp.where(lane // 32 == h, cand, jnp.zeros_like(cand))
            q_ref[u, h, :, WIDTH:] = bias
        return carry

    lax.fori_loop(0, OWN, one, 0)


def bias_columns(lead):
    r = lax.broadcasted_iota(jnp.int32, (SLOTS, PER_CHUNK), 0)
    b = lax.broadcasted_iota(jnp.int32, (SLOTS, PER_CHUNK), 1)
    repeat = jnp.where(r // CAP == b, 1.0, 0.0).astype(jnp.bfloat16)
    lead = jnp.dot(repeat, lead.astype(jnp.bfloat16), preferred_element_type=jnp.float32)
    slot = lax.rem(lax.broadcasted_iota(jnp.int32, (SLOTS, WIDTH), 0), CAP).astype(jnp.float32)
    follow = lax.rem(lax.broadcasted_iota(jnp.int32, (SLOTS, WIDTH), 1), 2)
    mine = jnp.where(follow == 1, slot - lead, lead - slot - 1.0) >= 0.0
    return jnp.where(mine, 0.0, -1e30).astype(jnp.bfloat16)


def pair_step(p, keys, bias, q_ref, m_ref, num_ref, den_ref):
    lane = lax.broadcasted_iota(jnp.int32, (SLOTS, WIDTH), 1)
    out_lane = lax.broadcasted_iota(jnp.int32, (ROWS, WIDTH), 1)
    key_ext = jnp.concatenate([keys, bias], axis=1)
    values = []
    for h in range(HEADS):
        own = lane // 32 == h
        ones = jnp.where(own, 1.0, 0.0).astype(jnp.bfloat16)
        values.append(jnp.concatenate([jnp.where(own, keys, jnp.zeros_like(keys)), ones], axis=1))
    for v in range(2):
        u = p * 2 + v
        total = None
        alpha = None
        for h in range(HEADS):
            s = lax.dot_general(q_ref[u, h], key_ext, (((1,), (1,)), ((), ())),
                                preferred_element_type=jnp.float32) * SCALE
            old = m_ref[u, h]
            new = jnp.maximum(old, jnp.max(s, axis=1, keepdims=True))
            m_ref[u, h] = new
            weights = jnp.exp2(s - jnp.concatenate([new, new], axis=1)).astype(jnp.bfloat16)
            part = jnp.dot(weights, values[h], preferred_element_type=jnp.float32)
            total = part if total is None else total + part
            shrink = jnp.exp2(old - new)
            alpha = shrink if alpha is None else jnp.where(out_lane // 32 == h, shrink, alpha)
        num_ref[u] = num_ref[u] * alpha + total[:, :WIDTH]
        den_ref[u] = den_ref[u] * alpha + total[:, WIDTH:]


def fused_kernel(hist_hbm, cats_ref, cand_cat_ref, cand_ref, w_in_ref, w_out_ref, out_ref,
                 pad_ref, cols_ref, events_ref, hid_ref, hist_ref, id_row_ref, ids_ref, key_ref, cnt_ref, send_ref, cnt_in_ref, recv_ref,
                 q_ref, m_ref, num_ref, den_ref, bias_ref,
                 hist_sems, line_send, line_recv, plane_send, plane_recv,
                 cnt_send, cnt_recv, data_send, data_recv):
    at = place()
    role, y, z, x = at
    base = y * 16 + z * 4
    me = role * 64 + base + x
    line, plane = line_peers(at), plane_peers(at)

    barrier = pltpu.get_barrier_semaphore()
    for r, s in plane + line:
        signal(barrier, r, s)
    loads = [
        pltpu.make_async_copy(hist_hbm.at[e], hist_ref.at[:, pl.ds(e * OWN, OWN), :], hist_sems.at[e])
        for e in range(E_DEV)
    ]
    for load in loads:
        load.start()
    id_row_ref[...] = distinct_row(cand_cat_ref[...].astype(jnp.float32))
    pl.semaphore_wait(barrier, len(line) + len(plane))

    for r, s in line:
        push(id_row_ref, ids_ref.at[pl.ds(me, 1)], line_send, line_recv, r, s)
    pltpu.make_async_copy(id_row_ref, ids_ref.at[pl.ds(me, 1)], line_recv).start()
    events_ref[...] = flat_events(cats_ref, pad_ref, cols_ref)
    fill_queries(cand_ref, q_ref)
    landed(ids_ref.at[pl.ds(0, 8)], line_recv)
    for r, s in plane:
        for half in range(2):
            rows = ids_ref.at[pl.ds(half * 64 + base, 4)]
            push(rows, rows, plane_send, plane_recv, r, s)
    m_ref[...] = jnp.full_like(m_ref, -3e38)
    num_ref[...] = jnp.zeros_like(num_ref)
    den_ref[...] = jnp.zeros_like(den_ref)

    def candidate_part(u, carry):
        hid_ref[u] = jnp.dot(cand_ref[u], w_in_ref[0:WIDTH, :], preferred_element_type=jnp.float32)
        return carry

    lax.fori_loop(0, OWN, candidate_part, 0)
    landed(ids_ref.at[pl.ds(0, 120)], plane_recv)

    key_ref[...], cnt_ref[...] = matched(ids_ref[...], events_ref[...])
    for load in loads:
        load.wait()
    rows = lax.broadcasted_iota(jnp.int32, (PAIRS * CAP, LANES), 0).astype(jnp.float32)

    def data_step(block, carry):
        peers = [partner(block, k, at) for k in range(BLOCK)]
        first = block * BLOCK
        chunk = block // (PER_CHUNK // BLOCK)
        for k, (r, s) in enumerate(peers):
            t = r * 64 + s
            pick = jnp.where(key_ref[pl.ds(t, 1), :] == rows, 1.0, 0.0).astype(jnp.bfloat16)
            packed = jnp.dot(pick, hist_ref[t], preferred_element_type=jnp.float32)
            send_ref[first + k] = packed.astype(jnp.bfloat16).reshape(PAIRS, CAP, WIDTH)
        for k, (r, s) in enumerate(peers):
            i = first + k
            cnt_src, cnt_dst = cnt_ref.at[pl.ds(r * 64 + s, 1)], cnt_in_ref.at[pl.ds(i, 1)]
            src, dst = send_ref.at[i], recv_ref.at[:, pl.ds(pl.multiple_of(i * CAP, CAP), CAP), :]

            def away(r=r, s=s, cnt_src=cnt_src, cnt_dst=cnt_dst, src=src, dst=dst):
                push(cnt_src, cnt_dst, cnt_send, cnt_recv.at[chunk], r, s)
                push(src, dst, data_send, data_recv.at[chunk], r, s)

            if k < BLOCK - 1:
                away()
            else:
                last = block == DEVS // BLOCK - 1
                pl.when(jnp.logical_not(last))(away)

                @pl.when(last)
                def _(cnt_src=cnt_src, cnt_dst=cnt_dst, src=src, dst=dst):
                    pltpu.make_async_copy(cnt_src, cnt_dst, cnt_recv.at[chunk]).start()
                    pltpu.make_async_copy(src, dst, data_recv.at[chunk]).start()
        return carry

    lax.fori_loop(0, DEVS // BLOCK, data_step, 0)

    def chunk_step(c, carry):
        counts = cnt_in_ref.at[pl.ds(c * PER_CHUNK, PER_CHUNK)]
        landed(counts, cnt_recv.at[c])
        slots = pl.ds(pl.multiple_of(c * SLOTS, SLOTS), SLOTS)
        landed(recv_ref.at[:, slots, :], data_recv.at[c])
        bias_ref[...] = bias_columns(counts[...])

        def one(p, carry):
            pair_step(p, recv_ref[p, slots, :], bias_ref[...], q_ref, m_ref, num_ref, den_ref)
            return carry

        return lax.fori_loop(0, PAIRS, one, carry)

    lax.fori_loop(0, CHUNKS, chunk_step, 0)

    def finish(u, carry):
        interest = (num_ref[u, 0:CANDS, :] / den_ref[u, 0:CANDS, :]).astype(jnp.bfloat16)
        hidden = hid_ref[u] + jnp.dot(interest, w_in_ref[WIDTH:, :], preferred_element_type=jnp.float32)
        hidden = (hidden / (1.0 + jnp.exp(-hidden))).astype(jnp.bfloat16)
        out_ref[u] = jnp.dot(hidden, w_out_ref[...], preferred_element_type=jnp.float32).astype(jnp.bfloat16)
        return carry

    lax.fori_loop(0, OWN, finish, 0)

    others = pl.ds(0, DEVS - 1)
    landed(send_ref.at[others], data_send)
    landed(cnt_ref.at[others], cnt_send)
    landed(ids_ref.at[pl.ds(0, 7)], line_send)
    landed(ids_ref.at[pl.ds(0, 120)], plane_send)


def local(history, event_cat, candidates, cand_cat, w_input, w_output):
    hist = history.transpose(1, 0, 2).reshape(E_DEV, DEVS, OWN, WIDTH)
    vm = pl.BlockSpec(memory_space=pltpu.VMEM)
    f32, bf16 = jnp.float32, jnp.bfloat16
    return pl.pallas_call(
        fused_kernel,
        out_shape=jax.ShapeDtypeStruct((OWN, CANDS, WIDTH), bf16),
        in_specs=[pl.BlockSpec(memory_space=pl.ANY), vm, vm, vm, vm, vm],
        out_specs=vm,
        scratch_shapes=[
            pltpu.VMEM((32, DEVS * OWN), jnp.int32),
            pltpu.VMEM((DEVS * OWN, WIDTH), jnp.int32),
            pltpu.VMEM((DEVS, LANES), f32),
            pltpu.VMEM((OWN, CANDS, HID), f32),
            pltpu.VMEM((DEVS, LANES, WIDTH), bf16),
            pltpu.VMEM((1, WIDTH), f32),
            pltpu.VMEM((DEVS, WIDTH), f32),
            pltpu.VMEM((DEVS, LANES), f32),
            pltpu.VMEM((DEVS, WIDTH), f32),
            pltpu.VMEM((DEVS, PAIRS, CAP, WIDTH), bf16),
            pltpu.VMEM((DEVS, WIDTH), f32),
            pltpu.VMEM((PAIRS, DEVS * CAP, WIDTH), bf16),
            pltpu.VMEM((OWN, HEADS, ROWS, 2 * WIDTH), bf16),
            pltpu.VMEM((OWN, HEADS, ROWS, WIDTH), f32),
            pltpu.VMEM((OWN, ROWS, WIDTH), f32),
            pltpu.VMEM((OWN, ROWS, WIDTH), f32),
            pltpu.VMEM((SLOTS, WIDTH), bf16),
            pltpu.SemaphoreType.DMA((E_DEV,)),
            pltpu.SemaphoreType.DMA, pltpu.SemaphoreType.DMA, pltpu.SemaphoreType.DMA, pltpu.SemaphoreType.DMA,
            pltpu.SemaphoreType.DMA, pltpu.SemaphoreType.DMA((CHUNKS,)),
            pltpu.SemaphoreType.DMA, pltpu.SemaphoreType.DMA((CHUNKS,)),
        ],
        compiler_params=pltpu.CompilerParams(collective_id=0, has_side_effects=True,
                                             vmem_limit_bytes=56 << 20),
        name="match_and_attend",
    )(hist, event_cat.T, cand_cat, candidates, w_input, w_output)


def solution(mesh):
    return jax.shard_map(
        local, mesh=mesh,
        in_specs=(P(None, AXES, None), P(None, AXES), P(AXES, None, None), P(AXES, None), P(), P()),
        out_specs=P(AXES, None, None), check_vma=False)
```

```python
import math

import jax
import jax.numpy as jnp
from jax import lax
from jax.experimental import pallas as pl
from jax.experimental.pallas import tpu as pltpu
from jax.sharding import PartitionSpec as P

AXES = ("role", "shard")
MESH = pl.DeviceIdType.MESH
DEVS = 128
SIDE = 4
E_DEV = 20
QCAT = 8
CAP = 8
OWN = 8
PAIRS = OWN // 2
LANES = E_DEV * OWN
WIDTH = 128


CANDS = 200
ROWS = 208
HEADS = 4
HID = 512
HEAD = WIDTH // HEADS
USER = HEADS * ROWS
COLS = 2 * USER
CHUNKS = 4
PER_CHUNK = DEVS // CHUNKS
SLOTS = PER_CHUNK * CAP
BLOCK = 16
SCALE = 32 ** -0.5 * math.log2(math.e)
FAR = (2, 3, 1, 0)


def place():
    role = lax.axis_index("role")
    shard = lax.axis_index("shard")
    return role, shard // 16, lax.rem(shard // 4, 4), lax.rem(shard, 4)


def partner(block, k, at):
    role, y, z, x = at
    r = lax.rem(role + 1 - lax.rem(block, 2), 2)
    dy, dz = FAR[k // 4], FAR[k % 4]
    px = lax.rem(x + block // 2 + 1 + 8 - dy - dz, 4)
    return r, lax.rem(y + dy, 4) * 16 + lax.rem(z + dz, 4) * 4 + px


def signal(sem, r, s):
    pl.semaphore_signal(sem, inc=1, device_id={"role": r, "shard": s}, device_id_type=MESH)


def push(src, dst, send_sem, recv_sem, r, s):
    pltpu.make_async_remote_copy(
        src_ref=src, dst_ref=dst, send_sem=send_sem, recv_sem=recv_sem,
        device_id={"role": r, "shard": s}, device_id_type=MESH).start()


def landed(ref, sem):
    pltpu.make_async_copy(ref, ref, sem).wait()


def line_peers(at):
    role, y, z, x = at
    return [(lax.rem(role + dr, 2), y * 16 + z * 4 + lax.rem(x + dx, 4))
            for dr in range(2) for dx in range(4) if dr or dx]


def plane_peers(at):
    role, y, z, x = at
    return [(role, lax.rem(y + dy, 4) * 16 + lax.rem(z + dz, 4) * 4 + x)
            for dy in FAR for dz in FAR if dy or dz]


def distinct_row(cats):
    lane = lax.broadcasted_iota(jnp.int32, (OWN, WIDTH), 1)
    sub = lax.broadcasted_iota(jnp.int32, (OWN, WIDTH), 0)
    spread = jnp.zeros((OWN, WIDTH), jnp.float32)
    last = jnp.full((OWN, 1), -1.0, jnp.float32)
    for k in range(QCAT):
        last = jnp.min(jnp.where(cats > last, cats, 4096.0), axis=1, keepdims=True)
        spot = (lax.rem(lane, 8) == sub) & (lax.rem(lane // 8, 8) == k)
        spread = jnp.where(spot, last, spread)
    row = jnp.sum(spread, axis=0, keepdims=True).astype(jnp.int32)
    low = lax.rem(row, 32)
    lane1 = lax.broadcasted_iota(jnp.int32, (1, WIDTH), 1)
    return jnp.where(lane1 < 64, row - low, low).astype(jnp.float32)


def flat_events(cats_ref, pad_ref, cols_ref):
    pad_ref[...] = jnp.zeros_like(pad_ref)
    pad_ref[0:E_DEV, :] = cats_ref[...]
    for j in range(OWN):
        cols_ref[j * WIDTH:(j + 1) * WIDTH, 0:32] = pad_ref[:, j * WIDTH:(j + 1) * WIDTH].T
    e = lax.broadcasted_iota(jnp.int32, (32, LANES), 0)
    lane = lax.broadcasted_iota(jnp.int32, (32, LANES), 1)
    flat = None
    for u in range(OWN):
        value = cols_ref[pl.ds(u, DEVS, stride=OWN), 0:32]
        low = lax.rem(value, 32)
        spot = jnp.where(lane == e * OWN + u, 1.0, 0.0).astype(jnp.bfloat16)
        for part in (value - low, low):
            moved = jnp.dot(part.astype(jnp.float32).astype(jnp.bfloat16), spot, preferred_element_type=jnp.float32)
            flat = moved if flat is None else flat + moved
    return flat


def matched(ids, events):
    ids = ids.astype(jnp.bfloat16)
    lane_i = lax.broadcasted_iota(jnp.int32, (DEVS, WIDTH), 1)
    er = lax.broadcasted_iota(jnp.int32, (WIDTH, LANES), 0)
    ec = lax.broadcasted_iota(jnp.int32, (WIDTH, LANES), 1)
    expand = jnp.where(lax.rem(er, 8) == lax.rem(ec, 8), 1.0, 0.0).astype(jnp.bfloat16)
    hit = None
    for k in range(QCAT):
        only = jnp.where(lax.rem(lane_i // 8, 8) == k, ids, jnp.zeros_like(ids))
        same = events == jnp.dot(only, expand, preferred_element_type=jnp.float32)
        hit = same if hit is None else hit | same
    hits = jnp.where(hit, 1.0, 0.0).astype(jnp.bfloat16)
    a = lax.broadcasted_iota(jnp.int32, (LANES, LANES), 0)
    b = lax.broadcasted_iota(jnp.int32, (LANES, LANES), 1)
    ua, ub = lax.rem(a, 8), lax.rem(b, 8)
    before = ((ua == ub) & (a < b)) | ((ua + 1 == ub) & (lax.rem(ub, 2) == 1))
    rank = jnp.dot(hits, jnp.where(before, 1.0, 0.0).astype(jnp.bfloat16), preferred_element_type=jnp.float32)
    lane_k = lax.broadcasted_iota(jnp.int32, (DEVS, LANES), 1)
    base = (lax.rem(lane_k, 8) // 2 * CAP).astype(jnp.float32)
    ca = lax.broadcasted_iota(jnp.int32, (LANES, WIDTH), 0)
    cb = lax.broadcasted_iota(jnp.int32, (LANES, WIDTH), 1)
    lead_of = jnp.where(lax.rem(ca, 8) == cb // 32 * 2, 1.0, 0.0).astype(jnp.bfloat16)
    lead = jnp.dot(hits, lead_of, preferred_element_type=jnp.float32)
    return jnp.where(hit, base + rank, -1.0), lead


def fill_queries(cand_ref, q_ref):
    row = lax.broadcasted_iota(jnp.int32, (WIDTH, ROWS), 0)

    def one(p, carry):
        parts = []
        for v in range(2):
            cand = cand_ref[p * 2 + v].astype(jnp.float32)
            cand = jnp.concatenate([cand, jnp.zeros((256 - CANDS, WIDTH), jnp.float32)], axis=0)
            turned = cand.T[:, :ROWS]
            for h in range(HEADS):
                parts.append(jnp.where(row // HEAD == h, turned, 0.0))
        q_ref[p] = jnp.concatenate(parts, axis=1).astype(jnp.bfloat16)
        return carry

    lax.fori_loop(0, PAIRS, one, 0)


def fill_owners(lead, mask_ref):
    a = lax.broadcasted_iota(jnp.int32, (WIDTH, PAIRS * WIDTH), 0)
    b = lax.broadcasted_iota(jnp.int32, (WIDTH, PAIRS * WIDTH), 1)
    wide = jnp.dot(lead.astype(jnp.bfloat16), jnp.where(a == b // WIDTH * 32, 1.0, 0.0).astype(jnp.bfloat16),
                   preferred_element_type=jnp.float32)
    r = lax.broadcasted_iota(jnp.int32, (SLOTS, PER_CHUNK), 0)
    c = lax.broadcasted_iota(jnp.int32, (SLOTS, PER_CHUNK), 1)
    tall = jnp.dot(jnp.where(r // CAP == c, 1.0, 0.0).astype(jnp.bfloat16), wide.astype(jnp.bfloat16),
                   preferred_element_type=jnp.float32)
    slot = lax.rem(lax.broadcasted_iota(jnp.int32, (SLOTS, WIDTH), 0), CAP).astype(jnp.float32)
    first = lax.broadcasted_iota(jnp.int32, (SLOTS, WIDTH), 1) < USER % WIDTH
    for p in range(PAIRS):
        one = jnp.where(slot < tall[:, p * WIDTH:(p + 1) * WIDTH], 1.0, 0.0)
        for i, kind in enumerate((one, jnp.where(first, one, 1.0 - one), 1.0 - one)):
            mask_ref[p, i] = kind.astype(mask_ref.dtype)


def by_tile(ref, p):
    whole = USER // WIDTH
    return jnp.concatenate([ref[p, 0]] * whole + [ref[p, 1]] + [ref[p, 2]] * whole, axis=1)


def value_rows(keys):
    turned = keys.astype(jnp.float32).T.astype(jnp.bfloat16)
    return jnp.concatenate([turned, jnp.ones((16, SLOTS), jnp.bfloat16)], axis=0)


def own_head(o):
    tiles = []
    for lo in range(0, COLS, WIDTH):
        h0, h1 = lo % USER // ROWS, (lo + WIDTH - 1) % USER // ROWS
        tile = o[HEAD * h0:HEAD * (h0 + 1), lo:lo + WIDTH]
        if h1 != h0:
            lane = lax.broadcasted_iota(jnp.int32, (HEAD, WIDTH), 1)
            tile = jnp.where(lane < ROWS - lo % ROWS, tile, o[HEAD * h1:HEAD * (h1 + 1), lo:lo + WIDTH])
        tiles.append(tile)
    return jnp.concatenate(tiles, axis=1)


def plain_step(p, keys, mask_ref, q_ref, acc_ref):
    s = jnp.dot(keys, q_ref[p], preferred_element_type=jnp.float32) * SCALE
    weights = jnp.exp2(s).astype(jnp.bfloat16) * by_tile(mask_ref, p)
    o = jnp.dot(value_rows(keys), weights, preferred_element_type=jnp.float32)
    acc_ref[p, 0:HEAD, :] += own_head(o)
    acc_ref[p, HEAD:, :] += o[WIDTH:WIDTH + 8]


def shifted_step(p, keys, mask_ref, q_ref, top_ref, acc_ref):
    s = jnp.dot(keys, q_ref[p], preferred_element_type=jnp.float32) * SCALE
    s = jnp.where(by_tile(mask_ref, p) > 0.5, s, -1e30)
    old = top_ref[p]
    new = jnp.maximum(old, jnp.max(s, axis=0, keepdims=True))
    top_ref[p] = new
    shrink = jnp.exp2(old - new)
    weights = jnp.exp2(s - new).astype(jnp.bfloat16)
    o = jnp.dot(value_rows(keys), weights, preferred_element_type=jnp.float32)
    acc_ref[p, 0:HEAD, :] = acc_ref[p, 0:HEAD, :] * shrink + own_head(o)
    acc_ref[p, HEAD:, :] = acc_ref[p, HEAD:, :] * shrink + o[WIDTH:WIDTH + 8]


def exchange_kernel(hist_hbm, cats_hbm, cand_cat_hbm, cand_hbm, acc_ref, recv_ref, cnt_in_ref,
                    cats_ref, cand_cat_ref, cand_ref,
                    pad_ref, cols_ref, events_ref, hist_ref, id_row_ref, ids_ref, key_ref, cnt_ref, send_ref,
                    q_ref, mask_ref,
                    small_sems, hist_sems, line_send, line_recv, plane_send, plane_recv,
                    cnt_send, cnt_recv, data_send, data_recv):
    at = place()
    role, y, z, x = at
    base = y * 16 + z * 4
    me = role * 64 + base + x
    line, plane = line_peers(at), plane_peers(at)

    barrier = pltpu.get_barrier_semaphore()
    for r, s in plane + line:
        signal(barrier, r, s)
    smalls = [
        pltpu.make_async_copy(src, dst, small_sems.at[n])
        for n, (src, dst) in enumerate((
            (cand_cat_hbm, cand_cat_ref), (cats_hbm, cats_ref), (cand_hbm, cand_ref)))
    ]
    for small in smalls:
        small.start()
    loads = [
        pltpu.make_async_copy(hist_hbm.at[e], hist_ref.at[:, pl.ds(e * OWN, OWN), :], hist_sems.at[e])
        for e in range(E_DEV)
    ]
    for load in loads:
        load.start()
    smalls[0].wait()
    id_row_ref[...] = distinct_row(cand_cat_ref[...].astype(jnp.float32))
    pl.semaphore_wait(barrier, len(line) + len(plane))

    for r, s in line:
        push(id_row_ref, ids_ref.at[pl.ds(me, 1)], line_send, line_recv, r, s)
    pltpu.make_async_copy(id_row_ref, ids_ref.at[pl.ds(me, 1)], line_recv).start()
    smalls[1].wait()
    events_ref[...] = flat_events(cats_ref, pad_ref, cols_ref)
    smalls[2].wait()
    fill_queries(cand_ref, q_ref)
    landed(ids_ref.at[pl.ds(0, 8)], line_recv)
    for r, s in plane:
        for half in range(2):
            rows = ids_ref.at[pl.ds(half * 64 + base, 4)]
            push(rows, rows, plane_send, plane_recv, r, s)
    acc_ref[...] = jnp.zeros_like(acc_ref)
    landed(ids_ref.at[pl.ds(0, 120)], plane_recv)

    key_ref[...], cnt_ref[...] = matched(ids_ref[...], events_ref[...])
    for load in loads:
        load.wait()
    rows = lax.broadcasted_iota(jnp.int32, (PAIRS * CAP, LANES), 0).astype(jnp.float32)

    def data_step(block, carry):
        peers = [partner(block, k, at) for k in range(BLOCK)]
        first = block * BLOCK
        chunk = block // (PER_CHUNK // BLOCK)
        for k, (r, s) in enumerate(peers):
            t = r * 64 + s
            pick = jnp.where(key_ref[pl.ds(t, 1), :] == rows, 1.0, 0.0).astype(jnp.bfloat16)
            packed = jnp.dot(pick, hist_ref[t], preferred_element_type=jnp.float32)
            send_ref[first + k] = packed.astype(jnp.bfloat16).reshape(PAIRS, CAP, WIDTH)
        for k, (r, s) in enumerate(peers):
            i = first + k
            cnt_src, cnt_dst = cnt_ref.at[pl.ds(r * 64 + s, 1)], cnt_in_ref.at[pl.ds(i, 1)]
            src, dst = send_ref.at[i], recv_ref.at[:, pl.ds(pl.multiple_of(i * CAP, CAP), CAP), :]

            def away(r=r, s=s, cnt_src=cnt_src, cnt_dst=cnt_dst, src=src, dst=dst):
                push(cnt_src, cnt_dst, cnt_send, cnt_recv.at[chunk], r, s)
                push(src, dst, data_send, data_recv.at[chunk], r, s)

            if k < BLOCK - 1:
                away()
            else:
                last = block == DEVS // BLOCK - 1
                pl.when(jnp.logical_not(last))(away)

                @pl.when(last)
                def _(cnt_src=cnt_src, cnt_dst=cnt_dst, src=src, dst=dst):
                    pltpu.make_async_copy(cnt_src, cnt_dst, cnt_recv.at[chunk]).start()
                    pltpu.make_async_copy(src, dst, data_recv.at[chunk]).start()
        return carry

    lax.fori_loop(0, DEVS // BLOCK, data_step, 0)

    def chunk_step(c, carry):
        counts = cnt_in_ref.at[pl.ds(c * PER_CHUNK, PER_CHUNK)]
        landed(counts, cnt_recv.at[c])
        slots = pl.ds(pl.multiple_of(c * SLOTS, SLOTS), SLOTS)
        landed(recv_ref.at[:, slots, :], data_recv.at[c])
        fill_owners(counts[...], mask_ref)
        for p in range(PAIRS):
            plain_step(p, recv_ref[p, slots, :], mask_ref, q_ref, acc_ref)
        return carry

    lax.fori_loop(0, CHUNKS, chunk_step, 0)

    others = pl.ds(0, DEVS - 1)
    landed(send_ref.at[others], data_send)
    landed(cnt_ref.at[others], cnt_send)
    landed(ids_ref.at[pl.ds(0, 7)], line_send)
    landed(ids_ref.at[pl.ds(0, 120)], plane_send)


def finish(sums_ref, cand_ref, w_in_ref, w_out_ref, stage_ref, out_hbm, sems):
    copies = []
    for p in range(PAIRS):
        share = sums_ref[p, 0:HEAD, :] * (1.0 / sums_ref[p, HEAD:HEAD + 1, :])
        turned = jnp.concatenate([share[:, lo:lo + WIDTH].T for lo in range(0, COLS, WIDTH)], axis=0)
        for v in range(2):
            u = p * 2 + v
            starts = [v * USER + h * ROWS for h in range(HEADS)]
            interest = jnp.concatenate([turned[lo:lo + ROWS] for lo in starts], axis=1)[0:CANDS]
            rows = jnp.concatenate([cand_ref[u], interest.astype(jnp.bfloat16)], axis=1)
            hidden = jnp.dot(rows, w_in_ref[...], preferred_element_type=jnp.float32)
            half = hidden * 0.5
            hidden = (half + half * jnp.tanh(half)).astype(jnp.bfloat16)
            stage_ref[u] = jnp.dot(hidden, w_out_ref[...], preferred_element_type=jnp.float32).astype(jnp.bfloat16)
        both = pl.ds(p * 2, 2)
        copies.append(pltpu.make_async_copy(stage_ref.at[both], out_hbm.at[both], sems.at[p]))
        copies[-1].start()
    for copy in copies:
        copy.wait()


def tower_kernel(acc_ref, cnt_ref, cand_ref, w_in_ref, w_out_ref, recv_hbm, out_hbm,
                 stage_ref, again_ref, recv_ref, q_ref, mask_ref, top_ref, sems):
    weights = acc_ref[:, HEAD:HEAD + 1, :]
    good = (weights > 2.0 ** -80) & (weights < 2.0 ** 110)
    safe = jnp.min(jnp.where(good, 1.0, 0.0)) > 0.5

    @pl.when(safe)
    def _():
        finish(acc_ref, cand_ref, w_in_ref, w_out_ref, stage_ref, out_hbm, sems)

    @pl.when(jnp.logical_not(safe))
    def _():
        pltpu.sync_copy(recv_hbm, recv_ref)
        fill_queries(cand_ref, q_ref)
        top_ref[...] = jnp.full_like(top_ref, -3e38)
        again_ref[...] = jnp.zeros_like(again_ref)

        def chunk_step(c, carry):
            fill_owners(cnt_ref[pl.ds(pl.multiple_of(c * PER_CHUNK, PER_CHUNK), PER_CHUNK), :], mask_ref)

            def one(p, carry):
                keys = recv_ref[p, pl.ds(pl.multiple_of(c * SLOTS, SLOTS), SLOTS), :]
                shifted_step(p, keys, mask_ref, q_ref, top_ref, again_ref)
                return carry

            return lax.fori_loop(0, PAIRS, one, carry)

        lax.fori_loop(0, CHUNKS, chunk_step, 0)
        finish(again_ref, cand_ref, w_in_ref, w_out_ref, stage_ref, out_hbm, sems)


def local(history, event_cat, candidates, cand_cat, w_input, w_output):
    hist = history.transpose(1, 0, 2).reshape(E_DEV, DEVS, OWN, WIDTH)
    vm = pl.BlockSpec(memory_space=pltpu.VMEM)
    hbm = pl.BlockSpec(memory_space=pltpu.HBM)
    f32, bf16, dma = jnp.float32, jnp.bfloat16, pltpu.SemaphoreType.DMA
    sums, slots, counts = pl.pallas_call(
        exchange_kernel,
        out_shape=(
            jax.ShapeDtypeStruct((PAIRS, HEAD + 8, COLS), f32),
            jax.ShapeDtypeStruct((PAIRS, DEVS * CAP, WIDTH), bf16),
            jax.ShapeDtypeStruct((DEVS, WIDTH), f32),
        ),
        in_specs=[hbm] * 4,
        out_specs=(vm, vm, vm),
        scratch_shapes=[
            pltpu.VMEM((E_DEV, DEVS * OWN), jnp.int32),
            pltpu.VMEM((OWN, CANDS), jnp.int32),
            pltpu.VMEM((OWN, CANDS, WIDTH), bf16),
            pltpu.VMEM((32, DEVS * OWN), jnp.int32),
            pltpu.VMEM((DEVS * OWN, WIDTH), jnp.int32),
            pltpu.VMEM((DEVS, LANES), f32),
            pltpu.VMEM((DEVS, LANES, WIDTH), bf16),
            pltpu.VMEM((1, WIDTH), f32),
            pltpu.VMEM((DEVS, WIDTH), f32),
            pltpu.VMEM((DEVS, LANES), f32),
            pltpu.VMEM((DEVS, WIDTH), f32),
            pltpu.VMEM((DEVS, PAIRS, CAP, WIDTH), bf16),
            pltpu.VMEM((PAIRS, WIDTH, COLS), bf16),
            pltpu.VMEM((PAIRS, 3, SLOTS, WIDTH), bf16),
            dma((3,)), dma((E_DEV,)), dma, dma, dma, dma, dma, dma((CHUNKS,)), dma, dma((CHUNKS,)),
        ],
        compiler_params=pltpu.CompilerParams(collective_id=0, has_side_effects=True, vmem_limit_bytes=40 << 20),
        name="match_and_attend",
    )(*(pltpu.with_memory_space_constraint(x, pltpu.HBM) for x in (hist, event_cat.T, cand_cat, candidates)))
    return pl.pallas_call(
        tower_kernel,
        out_shape=jax.ShapeDtypeStruct((OWN, CANDS, WIDTH), bf16),
        in_specs=[vm] * 5 + [pl.BlockSpec(memory_space=pl.ANY)],
        out_specs=hbm,
        scratch_shapes=[
            pltpu.VMEM((OWN, CANDS, WIDTH), bf16),
            pltpu.VMEM((PAIRS, HEAD + 8, COLS), f32),
            pltpu.VMEM((PAIRS, DEVS * CAP, WIDTH), bf16),
            pltpu.VMEM((PAIRS, WIDTH, COLS), bf16),
            pltpu.VMEM((PAIRS, 3, SLOTS, WIDTH), f32),
            pltpu.VMEM((PAIRS, 1, COLS), f32),
            dma((PAIRS,)),
        ],
        compiler_params=pltpu.CompilerParams(vmem_limit_bytes=40 << 20),
        name="tower",
    )(sums, counts, candidates, w_input, w_output, slots)


def solution(mesh):
    return jax.shard_map(
        local, mesh=mesh,
        in_specs=(P(None, AXES, None), P(None, AXES), P(AXES, None, None), P(AXES, None), P(), P()),
        out_specs=P(AXES, None, None), check_vma=False)
```

```python
import math

import jax
import jax.numpy as jnp
from jax import lax
from jax.experimental import pallas as pl
from jax.experimental.pallas import tpu as pltpu
from jax.sharding import PartitionSpec as P

AXES = ("role", "shard")
MESH = pl.DeviceIdType.MESH
DEVS = 128
SIDE = 4
E_DEV = 20
QCAT = 8
CAP = 8
OWN = 8
PAIRS = OWN // 2
LANES = E_DEV * OWN
WIDTH = 128


CANDS = 200
ROWS = 208
HEADS = 4
HID = 512
HEAD = WIDTH // HEADS
USER = HEADS * ROWS
COLS = 2 * USER
CHUNKS = 4
PER_CHUNK = DEVS // CHUNKS
SLOTS = PER_CHUNK * CAP
BLOCK = 16
SCALE = 32 ** -0.5 * math.log2(math.e)
FAR = (2, 3, 1, 0)


def place():
    role = lax.axis_index("role")
    shard = lax.axis_index("shard")
    return role, shard // 16, lax.rem(shard // 4, 4), lax.rem(shard, 4)


def partner(block, k, at):
    role, y, z, x = at
    r = lax.rem(role + 1 - lax.rem(block, 2), 2)
    dy, dz = FAR[k // 4], FAR[k % 4]
    px = lax.rem(x + block // 2 + 1 + 8 - dy - dz, 4)
    return r, lax.rem(y + dy, 4) * 16 + lax.rem(z + dz, 4) * 4 + px


def signal(sem, r, s):
    pl.semaphore_signal(sem, inc=1, device_id={"role": r, "shard": s}, device_id_type=MESH)


def push(src, dst, send_sem, recv_sem, r, s):
    pltpu.make_async_remote_copy(
        src_ref=src, dst_ref=dst, send_sem=send_sem, recv_sem=recv_sem,
        device_id={"role": r, "shard": s}, device_id_type=MESH).start()


def landed(ref, sem):
    pltpu.make_async_copy(ref, ref, sem).wait()


def line_peers(at):
    role, y, z, x = at
    return [(lax.rem(role + dr, 2), y * 16 + z * 4 + lax.rem(x + dx, 4))
            for dr in range(2) for dx in range(4) if dr or dx]


def plane_peers(at):
    role, y, z, x = at
    return [(role, lax.rem(y + dy, 4) * 16 + lax.rem(z + dz, 4) * 4 + x)
            for dy in FAR for dz in FAR if dy or dz]


def distinct_row(cats):
    lane = lax.broadcasted_iota(jnp.int32, (OWN, WIDTH), 1)
    sub = lax.broadcasted_iota(jnp.int32, (OWN, WIDTH), 0)
    spread = jnp.zeros((OWN, WIDTH), jnp.float32)
    last = jnp.full((OWN, 1), -1.0, jnp.float32)
    for k in range(QCAT):
        last = jnp.min(jnp.where(cats > last, cats, 4096.0), axis=1, keepdims=True)
        spot = (lax.rem(lane, 8) == sub) & (lax.rem(lane // 8, 8) == k)
        spread = jnp.where(spot, last, spread)
    row = jnp.sum(spread, axis=0, keepdims=True).astype(jnp.int32)
    low = lax.rem(row, 32)
    lane1 = lax.broadcasted_iota(jnp.int32, (1, WIDTH), 1)
    return jnp.where(lane1 < 64, row - low, low).astype(jnp.float32)


def flat_events(cats_ref, pad_ref, cols_ref):
    pad_ref[...] = jnp.zeros_like(pad_ref)
    pad_ref[0:E_DEV, :] = cats_ref[...]
    for j in range(OWN):
        cols_ref[j * WIDTH:(j + 1) * WIDTH, 0:32] = pad_ref[:, j * WIDTH:(j + 1) * WIDTH].T
    e = lax.broadcasted_iota(jnp.int32, (32, LANES), 0)
    lane = lax.broadcasted_iota(jnp.int32, (32, LANES), 1)
    flat = None
    for u in range(OWN):
        value = cols_ref[pl.ds(u, DEVS, stride=OWN), 0:32]
        low = lax.rem(value, 32)
        spot = jnp.where(lane == e * OWN + u, 1.0, 0.0).astype(jnp.bfloat16)
        for part in (value - low, low):
            moved = jnp.dot(part.astype(jnp.float32).astype(jnp.bfloat16), spot, preferred_element_type=jnp.float32)
            flat = moved if flat is None else flat + moved
    return flat


def matching_tables():
    er = lax.broadcasted_iota(jnp.int32, (WIDTH, LANES), 0)
    ec = lax.broadcasted_iota(jnp.int32, (WIDTH, LANES), 1)
    expand = lax.rem(er, 8) == lax.rem(ec, 8)
    a = lax.broadcasted_iota(jnp.int32, (LANES, LANES), 0)
    b = lax.broadcasted_iota(jnp.int32, (LANES, LANES), 1)
    ua, ub = lax.rem(a, 8), lax.rem(b, 8)
    before = ((ua == ub) & (a < b)) | ((ua + 1 == ub) & (lax.rem(ub, 2) == 1))
    ca = lax.broadcasted_iota(jnp.int32, (LANES, WIDTH), 0)
    cb = lax.broadcasted_iota(jnp.int32, (LANES, WIDTH), 1)
    lead_of = lax.rem(ca, 8) == cb // 32 * 2
    return [jnp.where(table, 1.0, 0.0).astype(jnp.bfloat16) for table in (expand, before, lead_of)]


def matched(ids, events, expand, before, lead_of):
    ids = ids.astype(jnp.bfloat16)
    lane_i = lax.broadcasted_iota(jnp.int32, (DEVS, WIDTH), 1)
    hit = None
    for k in range(QCAT):
        only = jnp.where(lax.rem(lane_i // 8, 8) == k, ids, jnp.zeros_like(ids))
        same = events == jnp.dot(only, expand, preferred_element_type=jnp.float32)
        hit = same if hit is None else hit | same
    hits = jnp.where(hit, 1.0, 0.0).astype(jnp.bfloat16)
    rank = jnp.dot(hits, before, preferred_element_type=jnp.float32)
    lane_k = lax.broadcasted_iota(jnp.int32, (DEVS, LANES), 1)
    base = (lax.rem(lane_k, 8) // 2 * CAP).astype(jnp.float32)
    lead = jnp.dot(hits, lead_of, preferred_element_type=jnp.float32)
    return jnp.where(hit, base + rank, -1.0), lead


def fill_queries(cand_ref, q_ref):
    row = lax.broadcasted_iota(jnp.int32, (WIDTH, ROWS), 0)

    def one(p, carry):
        parts = []
        for v in range(2):
            cand = cand_ref[p * 2 + v].astype(jnp.float32)
            cand = jnp.concatenate([cand, jnp.zeros((256 - CANDS, WIDTH), jnp.float32)], axis=0)
            turned = cand.T[:, :ROWS]
            for h in range(HEADS):
                parts.append(jnp.where(row // HEAD == h, turned, 0.0))
        q_ref[p] = jnp.concatenate(parts, axis=1).astype(jnp.bfloat16)
        return carry

    lax.fori_loop(0, PAIRS, one, 0)


def fill_owners(lead, mask_ref):
    a = lax.broadcasted_iota(jnp.int32, (WIDTH, PAIRS * WIDTH), 0)
    b = lax.broadcasted_iota(jnp.int32, (WIDTH, PAIRS * WIDTH), 1)
    wide = jnp.dot(lead.astype(jnp.bfloat16), jnp.where(a == b // WIDTH * 32, 1.0, 0.0).astype(jnp.bfloat16),
                   preferred_element_type=jnp.float32)
    r = lax.broadcasted_iota(jnp.int32, (SLOTS, PER_CHUNK), 0)
    c = lax.broadcasted_iota(jnp.int32, (SLOTS, PER_CHUNK), 1)
    tall = jnp.dot(jnp.where(r // CAP == c, 1.0, 0.0).astype(jnp.bfloat16), wide.astype(jnp.bfloat16),
                   preferred_element_type=jnp.float32)
    slot = lax.rem(lax.broadcasted_iota(jnp.int32, (SLOTS, WIDTH), 0), CAP).astype(jnp.float32)
    first = lax.broadcasted_iota(jnp.int32, (SLOTS, WIDTH), 1) < USER % WIDTH
    for p in range(PAIRS):
        one = jnp.where(slot < tall[:, p * WIDTH:(p + 1) * WIDTH], 1.0, 0.0)
        for i, kind in enumerate((one, jnp.where(first, one, 1.0 - one), 1.0 - one)):
            mask_ref[p, i] = kind.astype(mask_ref.dtype)


def by_tile(ref, p):
    whole = USER // WIDTH
    return jnp.concatenate([ref[p, 0]] * whole + [ref[p, 1]] + [ref[p, 2]] * whole, axis=1)


def value_rows(keys):
    turned = keys.astype(jnp.float32).T.astype(jnp.bfloat16)
    return jnp.concatenate([turned, jnp.ones((16, SLOTS), jnp.bfloat16)], axis=0)


def own_head(o):
    tiles = []
    for lo in range(0, COLS, WIDTH):
        h0, h1 = lo % USER // ROWS, (lo + WIDTH - 1) % USER // ROWS
        tile = o[HEAD * h0:HEAD * (h0 + 1), lo:lo + WIDTH]
        if h1 != h0:
            lane = lax.broadcasted_iota(jnp.int32, (HEAD, WIDTH), 1)
            tile = jnp.where(lane < ROWS - lo % ROWS, tile, o[HEAD * h1:HEAD * (h1 + 1), lo:lo + WIDTH])
        tiles.append(tile)
    return jnp.concatenate(tiles, axis=1)


def plain_step(p, keys, mask_ref, q_ref, acc_ref):
    s = jnp.dot(keys, q_ref[p], preferred_element_type=jnp.float32) * SCALE
    weights = jnp.exp2(s).astype(jnp.bfloat16) * by_tile(mask_ref, p)
    o = jnp.dot(value_rows(keys), weights, preferred_element_type=jnp.float32)
    acc_ref[p, 0:HEAD, :] += own_head(o)
    acc_ref[p, HEAD:, :] += o[WIDTH:WIDTH + 8]


def shifted_step(p, keys, mask_ref, q_ref, top_ref, acc_ref):
    s = jnp.dot(keys, q_ref[p], preferred_element_type=jnp.float32) * SCALE
    s = jnp.where(by_tile(mask_ref, p) > 0.5, s, -1e30)
    old = top_ref[p]
    new = jnp.maximum(old, jnp.max(s, axis=0, keepdims=True))
    top_ref[p] = new
    shrink = jnp.exp2(old - new)
    weights = jnp.exp2(s - new).astype(jnp.bfloat16)
    o = jnp.dot(value_rows(keys), weights, preferred_element_type=jnp.float32)
    acc_ref[p, 0:HEAD, :] = acc_ref[p, 0:HEAD, :] * shrink + own_head(o)
    acc_ref[p, HEAD:, :] = acc_ref[p, HEAD:, :] * shrink + o[WIDTH:WIDTH + 8]


def exchange_kernel(hist_hbm, cats_hbm, cand_cat_hbm, cand_hbm, w_in_hbm, acc_ref, recv_ref, cnt_in_ref, hid_ref,
                    cats_ref, cand_cat_ref, cand_ref, w_in_ref,
                    pad_ref, cols_ref, events_ref, hist_ref, id_row_ref, ids_ref, key_ref, cnt_ref, send_ref,
                    q_ref, mask_ref, expand_ref, before_ref, lead_of_ref,
                    small_sems, hist_sems, line_send, line_recv, plane_send, plane_recv,
                    cnt_send, cnt_recv, data_send, data_recv):
    at = place()
    role, y, z, x = at
    base = y * 16 + z * 4
    me = role * 64 + base + x
    line, plane = line_peers(at), plane_peers(at)

    barrier = pltpu.get_barrier_semaphore()
    for r, s in plane + line:
        signal(barrier, r, s)
    smalls = [
        pltpu.make_async_copy(src, dst, small_sems.at[n])
        for n, (src, dst) in enumerate((
            (cand_cat_hbm, cand_cat_ref), (cats_hbm, cats_ref), (cand_hbm, cand_ref),
            (w_in_hbm.at[pl.ds(0, WIDTH)], w_in_ref)))
    ]
    for small in smalls:
        small.start()
    loads = [
        pltpu.make_async_copy(hist_hbm.at[e], hist_ref.at[:, pl.ds(e * OWN, OWN), :], hist_sems.at[e])
        for e in range(E_DEV)
    ]
    for load in loads:
        load.start()
    smalls[0].wait()
    id_row_ref[...] = distinct_row(cand_cat_ref[...].astype(jnp.float32))
    pl.semaphore_wait(barrier, len(line) + len(plane))

    for r, s in line:
        push(id_row_ref, ids_ref.at[pl.ds(me, 1)], line_send, line_recv, r, s)
    pltpu.make_async_copy(id_row_ref, ids_ref.at[pl.ds(me, 1)], line_recv).start()
    smalls[1].wait()
    events_ref[...] = flat_events(cats_ref, pad_ref, cols_ref)
    smalls[2].wait()
    fill_queries(cand_ref, q_ref)
    landed(ids_ref.at[pl.ds(0, 8)], line_recv)
    for r, s in plane:
        for half in range(2):
            rows = ids_ref.at[pl.ds(half * 64 + base, 4)]
            push(rows, rows, plane_send, plane_recv, r, s)
    acc_ref[...] = jnp.zeros_like(acc_ref)
    expand_ref[...], before_ref[...], lead_of_ref[...] = matching_tables()
    smalls[3].wait()

    def candidate_part(u, carry):
        hid_ref[u, 0:CANDS, :] = jnp.dot(cand_ref[u], w_in_ref[...], preferred_element_type=jnp.float32)
        return carry

    lax.fori_loop(0, OWN, candidate_part, 0)
    for load in loads:
        load.wait()
    landed(ids_ref.at[pl.ds(0, 120)], plane_recv)

    key_ref[...], cnt_ref[...] = matched(ids_ref[...], events_ref[...], expand_ref[...], before_ref[...], lead_of_ref[...])
    rows = lax.broadcasted_iota(jnp.int32, (PAIRS * CAP, LANES), 0).astype(jnp.float32)

    def data_step(block, carry):
        peers = [partner(block, k, at) for k in range(BLOCK)]
        first = block * BLOCK
        chunk = block // (PER_CHUNK // BLOCK)
        for k, (r, s) in enumerate(peers):
            t = r * 64 + s
            pick = jnp.where(key_ref[pl.ds(t, 1), :] == rows, 1.0, 0.0).astype(jnp.bfloat16)
            packed = jnp.dot(pick, hist_ref[t], preferred_element_type=jnp.float32)
            send_ref[first + k] = packed.astype(jnp.bfloat16).reshape(PAIRS, CAP, WIDTH)
        for k, (r, s) in enumerate(peers):
            i = first + k
            cnt_src, cnt_dst = cnt_ref.at[pl.ds(r * 64 + s, 1)], cnt_in_ref.at[pl.ds(i, 1)]
            src, dst = send_ref.at[i], recv_ref.at[:, pl.ds(pl.multiple_of(i * CAP, CAP), CAP), :]

            def away(r=r, s=s, cnt_src=cnt_src, cnt_dst=cnt_dst, src=src, dst=dst):
                push(cnt_src, cnt_dst, cnt_send, cnt_recv.at[chunk], r, s)
                push(src, dst, data_send, data_recv.at[chunk], r, s)

            if k < BLOCK - 1:
                away()
            else:
                last = block == DEVS // BLOCK - 1
                pl.when(jnp.logical_not(last))(away)

                @pl.when(last)
                def _(cnt_src=cnt_src, cnt_dst=cnt_dst, src=src, dst=dst):
                    pltpu.make_async_copy(cnt_src, cnt_dst, cnt_recv.at[chunk]).start()
                    pltpu.make_async_copy(src, dst, data_recv.at[chunk]).start()
        return carry

    lax.fori_loop(0, DEVS // BLOCK, data_step, 0)

    def chunk_step(c, carry):
        counts = cnt_in_ref.at[pl.ds(c * PER_CHUNK, PER_CHUNK)]
        landed(counts, cnt_recv.at[c])
        slots = pl.ds(pl.multiple_of(c * SLOTS, SLOTS), SLOTS)
        fill_owners(counts[...], mask_ref)
        landed(recv_ref.at[:, slots, :], data_recv.at[c])
        for p in range(PAIRS):
            plain_step(p, recv_ref[p, slots, :], mask_ref, q_ref, acc_ref)
        return carry

    lax.fori_loop(0, CHUNKS, chunk_step, 0)

    others = pl.ds(0, DEVS - 1)
    landed(send_ref.at[others], data_send)
    landed(cnt_ref.at[others], cnt_send)
    landed(ids_ref.at[pl.ds(0, 7)], line_send)
    landed(ids_ref.at[pl.ds(0, 120)], plane_send)


def finish(sums_ref, hid_ref, w_in_ref, w_out_ref, stage_ref, out_hbm, sems):
    copies = []
    for p in range(PAIRS):
        share = sums_ref[p, 0:HEAD, :] * (1.0 / sums_ref[p, HEAD:HEAD + 1, :])
        turned = jnp.concatenate([share[:, lo:lo + WIDTH].T for lo in range(0, COLS, WIDTH)], axis=0)
        users = []
        for v in range(2):
            starts = [v * USER + h * ROWS for h in range(HEADS)]
            users.append(jnp.concatenate([turned[lo:lo + ROWS] for lo in starts], axis=1))
        interest = jnp.concatenate(users, axis=0).astype(jnp.bfloat16)
        hidden = jnp.dot(interest, w_in_ref[WIDTH:, :], preferred_element_type=jnp.float32)
        hidden = hidden + hid_ref[2 * p:2 * p + 2].reshape(2 * ROWS, HID)
        half = hidden * 0.5
        hidden = (half + half * jnp.tanh(half)).astype(jnp.bfloat16)
        result = jnp.dot(hidden, w_out_ref[...], preferred_element_type=jnp.float32).astype(jnp.bfloat16)
        stage_ref[2 * p:2 * p + 2] = result.reshape(2, ROWS, WIDTH)
        both = pl.ds(p * 2, 2)
        copies.append(pltpu.make_async_copy(stage_ref.at[both, 0:CANDS], out_hbm.at[both], sems.at[p]))
        copies[-1].start()
    for copy in copies:
        copy.wait()


def tower_kernel(acc_ref, cnt_ref, hid_ref, w_in_ref, w_out_ref, recv_hbm, cand_hbm, out_hbm,
                 stage_ref, again_ref, recv_ref, cand_ref, q_ref, mask_ref, top_ref, sems):
    finish(acc_ref, hid_ref, w_in_ref, w_out_ref, stage_ref, out_hbm, sems)
    weights = acc_ref[:, HEAD:HEAD + 1, :]
    good = (weights > 2.0 ** -80) & (weights < 2.0 ** 110)

    @pl.when(jnp.min(jnp.where(good, 1.0, 0.0)) < 0.5)
    def _():
        pltpu.sync_copy(recv_hbm, recv_ref)
        pltpu.sync_copy(cand_hbm, cand_ref)
        fill_queries(cand_ref, q_ref)
        top_ref[...] = jnp.full_like(top_ref, -3e38)
        again_ref[...] = jnp.zeros_like(again_ref)

        def chunk_step(c, carry):
            fill_owners(cnt_ref[pl.ds(pl.multiple_of(c * PER_CHUNK, PER_CHUNK), PER_CHUNK), :], mask_ref)

            def one(p, carry):
                keys = recv_ref[p, pl.ds(pl.multiple_of(c * SLOTS, SLOTS), SLOTS), :]
                shifted_step(p, keys, mask_ref, q_ref, top_ref, again_ref)
                return carry

            return lax.fori_loop(0, PAIRS, one, carry)

        lax.fori_loop(0, CHUNKS, chunk_step, 0)
        finish(again_ref, hid_ref, w_in_ref, w_out_ref, stage_ref, out_hbm, sems)


def local(history, event_cat, candidates, cand_cat, w_input, w_output):
    hist = history.transpose(1, 0, 2).reshape(E_DEV, DEVS, OWN, WIDTH)
    vm = pl.BlockSpec(memory_space=pltpu.VMEM)
    hbm = pl.BlockSpec(memory_space=pltpu.HBM)
    f32, bf16, dma = jnp.float32, jnp.bfloat16, pltpu.SemaphoreType.DMA
    sums, slots, counts, hidden = pl.pallas_call(
        exchange_kernel,
        out_shape=(
            jax.ShapeDtypeStruct((PAIRS, HEAD + 8, COLS), f32),
            jax.ShapeDtypeStruct((PAIRS, DEVS * CAP, WIDTH), bf16),
            jax.ShapeDtypeStruct((DEVS, WIDTH), f32),
            jax.ShapeDtypeStruct((OWN, ROWS, HID), f32),
        ),
        in_specs=[hbm] * 5,
        out_specs=(vm, vm, vm, vm),
        scratch_shapes=[
            pltpu.VMEM((E_DEV, DEVS * OWN), jnp.int32),
            pltpu.VMEM((OWN, CANDS), jnp.int32),
            pltpu.VMEM((OWN, CANDS, WIDTH), bf16),
            pltpu.VMEM((WIDTH, HID), bf16),
            pltpu.VMEM((32, DEVS * OWN), jnp.int32),
            pltpu.VMEM((DEVS * OWN, WIDTH), jnp.int32),
            pltpu.VMEM((DEVS, LANES), f32),
            pltpu.VMEM((DEVS, LANES, WIDTH), bf16),
            pltpu.VMEM((1, WIDTH), f32),
            pltpu.VMEM((DEVS, WIDTH), f32),
            pltpu.VMEM((DEVS, LANES), f32),
            pltpu.VMEM((DEVS, WIDTH), f32),
            pltpu.VMEM((DEVS, PAIRS, CAP, WIDTH), bf16),
            pltpu.VMEM((PAIRS, WIDTH, COLS), bf16),
            pltpu.VMEM((PAIRS, 3, SLOTS, WIDTH), bf16),
            pltpu.VMEM((WIDTH, LANES), bf16),
            pltpu.VMEM((LANES, LANES), bf16),
            pltpu.VMEM((LANES, WIDTH), bf16),
            dma((4,)), dma((E_DEV,)), dma, dma, dma, dma, dma, dma((CHUNKS,)), dma, dma((CHUNKS,)),
        ],
        compiler_params=pltpu.CompilerParams(collective_id=0, has_side_effects=True, vmem_limit_bytes=40 << 20),
        name="match_and_attend",
    )(*(pltpu.with_memory_space_constraint(x, pltpu.HBM) for x in (hist, event_cat.T, cand_cat, candidates, w_input)))
    return pl.pallas_call(
        tower_kernel,
        out_shape=jax.ShapeDtypeStruct((OWN, CANDS, WIDTH), bf16),
        in_specs=[vm] * 5 + [pl.BlockSpec(memory_space=pl.ANY)] * 2,
        out_specs=hbm,
        scratch_shapes=[
            pltpu.VMEM((OWN, ROWS, WIDTH), bf16),
            pltpu.VMEM((PAIRS, HEAD + 8, COLS), f32),
            pltpu.VMEM((PAIRS, DEVS * CAP, WIDTH), bf16),
            pltpu.VMEM((OWN, CANDS, WIDTH), bf16),
            pltpu.VMEM((PAIRS, WIDTH, COLS), bf16),
            pltpu.VMEM((PAIRS, 3, SLOTS, WIDTH), f32),
            pltpu.VMEM((PAIRS, 1, COLS), f32),
            dma((PAIRS,)),
        ],
        compiler_params=pltpu.CompilerParams(vmem_limit_bytes=40 << 20),
        name="tower",
    )(sums, counts, hidden, w_input, w_output, slots, candidates)


def solution(mesh):
    return jax.shard_map(
        local, mesh=mesh,
        in_specs=(P(None, AXES, None), P(None, AXES), P(AXES, None, None), P(AXES, None), P(), P()),
        out_specs=P(AXES, None, None), check_vma=False)
```

```python
import math

import jax
import jax.numpy as jnp
from jax import lax
from jax.experimental import pallas as pl
from jax.experimental.pallas import tpu as pltpu
from jax.sharding import PartitionSpec as P

AXES = ("role", "shard")
MESH = pl.DeviceIdType.MESH
DEVS = 128
SIDE = 4
E_DEV = 20
QCAT = 8
CAP = 8
OWN = 8
PAIRS = OWN // 2
LANES = E_DEV * OWN
WIDTH = 128


CANDS = 200
ROWS = 208
HEADS = 4
HID = 512
HEAD = WIDTH // HEADS
USER = HEADS * ROWS
COLS = 2 * USER
CHUNKS = 4
PER_CHUNK = DEVS // CHUNKS
SLOTS = PER_CHUNK * CAP
BLOCK = 16
SCALE = 32 ** -0.5 * math.log2(math.e)
FAR = (2, 3, 1, 0)


def place():
    role = lax.axis_index("role")
    shard = lax.axis_index("shard")
    return role, shard // 16, lax.rem(shard // 4, 4), lax.rem(shard, 4)


def partner(block, k, at):
    role, y, z, x = at
    r = lax.rem(role + 1 - lax.rem(block, 2), 2)
    dy, dz = FAR[k // 4], FAR[k % 4]
    px = lax.rem(x + block // 2 + 1 + 8 - dy - dz, 4)
    return r, lax.rem(y + dy, 4) * 16 + lax.rem(z + dz, 4) * 4 + px


def signal(sem, r, s):
    pl.semaphore_signal(sem, inc=1, device_id={"role": r, "shard": s}, device_id_type=MESH)


def push(src, dst, send_sem, recv_sem, r, s):
    pltpu.make_async_remote_copy(
        src_ref=src, dst_ref=dst, send_sem=send_sem, recv_sem=recv_sem,
        device_id={"role": r, "shard": s}, device_id_type=MESH).start()


def landed(ref, sem):
    pltpu.make_async_copy(ref, ref, sem).wait()


def line_peers(at):
    role, y, z, x = at
    return [(lax.rem(role + dr, 2), y * 16 + z * 4 + lax.rem(x + dx, 4))
            for dr in range(2) for dx in range(4) if dr or dx]


def plane_peers(at):
    role, y, z, x = at
    return [(role, lax.rem(y + dy, 4) * 16 + lax.rem(z + dz, 4) * 4 + x)
            for dy in FAR for dz in FAR if dy or dz]


def distinct_row(cats):
    lane = lax.broadcasted_iota(jnp.int32, (OWN, WIDTH), 1)
    sub = lax.broadcasted_iota(jnp.int32, (OWN, WIDTH), 0)
    spread = jnp.zeros((OWN, WIDTH), jnp.float32)
    last = jnp.full((OWN, 1), -1.0, jnp.float32)
    for k in range(QCAT):
        last = jnp.min(jnp.where(cats > last, cats, 4096.0), axis=1, keepdims=True)
        spot = (lax.rem(lane, 8) == sub) & (lax.rem(lane // 8, 8) == k)
        spread = jnp.where(spot, last, spread)
    row = jnp.sum(spread, axis=0, keepdims=True).astype(jnp.int32)
    low = lax.rem(row, 32)
    lane1 = lax.broadcasted_iota(jnp.int32, (1, WIDTH), 1)
    return jnp.where(lane1 < 64, row - low, low).astype(jnp.float32)


def flat_events(cats_ref, pad_ref, cols_ref):
    pad_ref[...] = jnp.zeros_like(pad_ref)
    pad_ref[0:E_DEV, :] = cats_ref[...]
    for j in range(OWN):
        cols_ref[j * WIDTH:(j + 1) * WIDTH, 0:32] = pad_ref[:, j * WIDTH:(j + 1) * WIDTH].T
    e = lax.broadcasted_iota(jnp.int32, (32, LANES), 0)
    lane = lax.broadcasted_iota(jnp.int32, (32, LANES), 1)
    flat = None
    for u in range(OWN):
        value = cols_ref[pl.ds(u, DEVS, stride=OWN), 0:32]
        low = lax.rem(value, 32)
        spot = jnp.where(lane == e * OWN + u, 1.0, 0.0).astype(jnp.bfloat16)
        for part in (value - low, low):
            moved = jnp.dot(part.astype(jnp.float32).astype(jnp.bfloat16), spot, preferred_element_type=jnp.float32)
            flat = moved if flat is None else flat + moved
    return flat


def matching_tables():
    er = lax.broadcasted_iota(jnp.int32, (WIDTH, LANES), 0)
    ec = lax.broadcasted_iota(jnp.int32, (WIDTH, LANES), 1)
    expand = lax.rem(er, 8) == lax.rem(ec, 8)
    a = lax.broadcasted_iota(jnp.int32, (LANES, LANES), 0)
    b = lax.broadcasted_iota(jnp.int32, (LANES, LANES), 1)
    ua, ub = lax.rem(a, 8), lax.rem(b, 8)
    before = ((ua == ub) & (a < b)) | ((ua + 1 == ub) & (lax.rem(ub, 2) == 1))
    ca = lax.broadcasted_iota(jnp.int32, (LANES, WIDTH), 0)
    cb = lax.broadcasted_iota(jnp.int32, (LANES, WIDTH), 1)
    lead_of = lax.rem(ca, 8) == cb // 32 * 2
    return [jnp.where(table, 1.0, 0.0).astype(jnp.bfloat16) for table in (expand, before, lead_of)]


def matched(ids, events, expand, before, lead_of):
    ids = ids.astype(jnp.bfloat16)
    lane_i = lax.broadcasted_iota(jnp.int32, (DEVS, WIDTH), 1)
    hit = None
    for k in range(QCAT):
        only = jnp.where(lax.rem(lane_i // 8, 8) == k, ids, jnp.zeros_like(ids))
        same = events == jnp.dot(only, expand, preferred_element_type=jnp.float32)
        hit = same if hit is None else hit | same
    hits = jnp.where(hit, 1.0, 0.0).astype(jnp.bfloat16)
    rank = jnp.dot(hits, before, preferred_element_type=jnp.float32)
    lane_k = lax.broadcasted_iota(jnp.int32, (DEVS, LANES), 1)
    base = (lax.rem(lane_k, 8) // 2 * CAP).astype(jnp.float32)
    lead = jnp.dot(hits, lead_of, preferred_element_type=jnp.float32)
    return jnp.where(hit, base + rank, -1.0), lead


def fill_queries(cand_ref, q_ref):
    row = lax.broadcasted_iota(jnp.int32, (WIDTH, ROWS), 0)

    def one(p, carry):
        parts = []
        for v in range(2):
            cand = cand_ref[p * 2 + v].astype(jnp.float32)
            cand = jnp.concatenate([cand, jnp.zeros((256 - CANDS, WIDTH), jnp.float32)], axis=0)
            turned = cand.T[:, :ROWS]
            for h in range(HEADS):
                parts.append(jnp.where(row // HEAD == h, turned, 0.0))
        q_ref[p] = jnp.concatenate(parts, axis=1).astype(jnp.bfloat16)
        return carry

    lax.fori_loop(0, PAIRS, one, 0)


def fill_owners(lead, mask_ref):
    a = lax.broadcasted_iota(jnp.int32, (WIDTH, PAIRS * WIDTH), 0)
    b = lax.broadcasted_iota(jnp.int32, (WIDTH, PAIRS * WIDTH), 1)
    wide = jnp.dot(lead.astype(jnp.bfloat16), jnp.where(a == b // WIDTH * 32, 1.0, 0.0).astype(jnp.bfloat16),
                   preferred_element_type=jnp.float32)
    r = lax.broadcasted_iota(jnp.int32, (SLOTS, PER_CHUNK), 0)
    c = lax.broadcasted_iota(jnp.int32, (SLOTS, PER_CHUNK), 1)
    tall = jnp.dot(jnp.where(r // CAP == c, 1.0, 0.0).astype(jnp.bfloat16), wide.astype(jnp.bfloat16),
                   preferred_element_type=jnp.float32)
    slot = lax.rem(lax.broadcasted_iota(jnp.int32, (SLOTS, WIDTH), 0), CAP).astype(jnp.float32)
    first = lax.broadcasted_iota(jnp.int32, (SLOTS, WIDTH), 1) < USER % WIDTH
    for p in range(PAIRS):
        one = jnp.where(slot < tall[:, p * WIDTH:(p + 1) * WIDTH], 1.0, 0.0)
        for i, kind in enumerate((one, jnp.where(first, one, 1.0 - one), 1.0 - one)):
            mask_ref[p, i] = kind.astype(mask_ref.dtype)


def by_tile(ref, p):
    whole = USER // WIDTH
    return jnp.concatenate([ref[p, 0]] * whole + [ref[p, 1]] + [ref[p, 2]] * whole, axis=1)


def value_rows(keys):
    turned = keys.astype(jnp.float32).T.astype(jnp.bfloat16)
    return jnp.concatenate([turned, jnp.ones((16, SLOTS), jnp.bfloat16)], axis=0)


def own_head(o):
    tiles = []
    for lo in range(0, COLS, WIDTH):
        h0, h1 = lo % USER // ROWS, (lo + WIDTH - 1) % USER // ROWS
        tile = o[HEAD * h0:HEAD * (h0 + 1), lo:lo + WIDTH]
        if h1 != h0:
            lane = lax.broadcasted_iota(jnp.int32, (HEAD, WIDTH), 1)
            tile = jnp.where(lane < ROWS - lo % ROWS, tile, o[HEAD * h1:HEAD * (h1 + 1), lo:lo + WIDTH])
        tiles.append(tile)
    return jnp.concatenate(tiles, axis=1)


def plain_step(p, keys, mask_ref, q_ref, acc_ref):
    s = jnp.dot(keys, q_ref[p], preferred_element_type=jnp.float32) * SCALE
    weights = jnp.exp2(s).astype(jnp.bfloat16) * by_tile(mask_ref, p)
    o = jnp.dot(value_rows(keys), weights, preferred_element_type=jnp.float32)
    acc_ref[p, 0:HEAD, :] += own_head(o)
    acc_ref[p, HEAD:, :] += o[WIDTH:WIDTH + 8]


def shifted_step(p, keys, mask_ref, q_ref, top_ref, acc_ref):
    s = jnp.dot(keys, q_ref[p], preferred_element_type=jnp.float32) * SCALE
    s = jnp.where(by_tile(mask_ref, p) > 0.5, s, -1e30)
    old = top_ref[p]
    new = jnp.maximum(old, jnp.max(s, axis=0, keepdims=True))
    top_ref[p] = new
    shrink = jnp.exp2(old - new)
    weights = jnp.exp2(s - new).astype(jnp.bfloat16)
    o = jnp.dot(value_rows(keys), weights, preferred_element_type=jnp.float32)
    acc_ref[p, 0:HEAD, :] = acc_ref[p, 0:HEAD, :] * shrink + own_head(o)
    acc_ref[p, HEAD:, :] = acc_ref[p, HEAD:, :] * shrink + o[WIDTH:WIDTH + 8]


def exchange_kernel(hist_hbm, cats_hbm, cand_cat_hbm, cand_hbm, w_in_hbm, acc_ref, recv_ref, cnt_in_ref, hid_ref,
                    cats_ref, cand_cat_ref, cand_ref, w_in_ref,
                    pad_ref, cols_ref, events_ref, hist_ref, id_row_ref, ids_ref, key_ref, cnt_ref, send_ref,
                    q_ref, mask_ref, expand_ref, before_ref, lead_of_ref,
                    small_sems, hist_sems, line_send, line_recv, plane_send, plane_recv,
                    cnt_send, cnt_recv, data_send, data_recv):
    at = place()
    role, y, z, x = at
    base = y * 16 + z * 4
    me = role * 64 + base + x
    line, plane = line_peers(at), plane_peers(at)

    barrier = pltpu.get_barrier_semaphore()
    for r, s in plane + line:
        signal(barrier, r, s)
    smalls = [
        pltpu.make_async_copy(src, dst, small_sems.at[n])
        for n, (src, dst) in enumerate((
            (cand_cat_hbm, cand_cat_ref), (cats_hbm, cats_ref), (cand_hbm, cand_ref),
            (w_in_hbm.at[pl.ds(0, WIDTH)], w_in_ref)))
    ]
    for small in smalls:
        small.start()
    loads = [
        pltpu.make_async_copy(hist_hbm.at[e], hist_ref.at[:, pl.ds(e * OWN, OWN), :], hist_sems.at[e])
        for e in range(E_DEV)
    ]
    for load in loads:
        load.start()
    smalls[0].wait()
    id_row_ref[...] = distinct_row(cand_cat_ref[...].astype(jnp.float32))
    pl.semaphore_wait(barrier, len(line) + len(plane))

    for r, s in line:
        push(id_row_ref, ids_ref.at[pl.ds(me, 1)], line_send, line_recv, r, s)
    pltpu.make_async_copy(id_row_ref, ids_ref.at[pl.ds(me, 1)], line_recv).start()
    smalls[1].wait()
    events_ref[...] = flat_events(cats_ref, pad_ref, cols_ref)
    smalls[2].wait()
    fill_queries(cand_ref, q_ref)
    landed(ids_ref.at[pl.ds(0, 8)], line_recv)
    for r, s in plane:
        for half in range(2):
            rows = ids_ref.at[pl.ds(half * 64 + base, 4)]
            push(rows, rows, plane_send, plane_recv, r, s)
    acc_ref[...] = jnp.zeros_like(acc_ref)
    expand_ref[...], before_ref[...], lead_of_ref[...] = matching_tables()
    smalls[3].wait()

    def candidate_part(u, carry):
        hid_ref[u, 0:CANDS, :] = jnp.dot(cand_ref[u], w_in_ref[...], preferred_element_type=jnp.float32)
        return carry

    lax.fori_loop(0, OWN, candidate_part, 0)
    for load in loads:
        load.wait()
    landed(ids_ref.at[pl.ds(0, 120)], plane_recv)

    key_ref[...], cnt_ref[...] = matched(ids_ref[...], events_ref[...], expand_ref[...], before_ref[...], lead_of_ref[...])
    rows = lax.broadcasted_iota(jnp.int32, (PAIRS * CAP, LANES), 0).astype(jnp.float32)

    def data_step(block, carry):
        peers = [partner(block, k, at) for k in range(BLOCK)]
        first = block * BLOCK
        chunk = block // (PER_CHUNK // BLOCK)
        for k, (r, s) in enumerate(peers):
            t = r * 64 + s
            pick = jnp.where(key_ref[pl.ds(t, 1), :] == rows, 1.0, 0.0).astype(jnp.bfloat16)
            packed = jnp.dot(pick, hist_ref[t], preferred_element_type=jnp.float32)
            send_ref[first + k] = packed.astype(jnp.bfloat16).reshape(PAIRS, CAP, WIDTH)
        for k, (r, s) in enumerate(peers):
            i = first + k
            cnt_src, cnt_dst = cnt_ref.at[pl.ds(r * 64 + s, 1)], cnt_in_ref.at[pl.ds(i, 1)]
            src, dst = send_ref.at[i], recv_ref.at[:, pl.ds(pl.multiple_of(i * CAP, CAP), CAP), :]

            def away(r=r, s=s, cnt_src=cnt_src, cnt_dst=cnt_dst, src=src, dst=dst):
                push(cnt_src, cnt_dst, cnt_send, cnt_recv.at[chunk], r, s)
                push(src, dst, data_send, data_recv.at[chunk], r, s)

            if k < BLOCK - 1:
                away()
            else:
                last = block == DEVS // BLOCK - 1
                pl.when(jnp.logical_not(last))(away)

                @pl.when(last)
                def _(cnt_src=cnt_src, cnt_dst=cnt_dst, src=src, dst=dst):
                    pltpu.make_async_copy(cnt_src, cnt_dst, cnt_recv.at[chunk]).start()
                    pltpu.make_async_copy(src, dst, data_recv.at[chunk]).start()
        return carry

    lax.fori_loop(0, DEVS // BLOCK, data_step, 0)

    def chunk_step(c, carry):
        counts = cnt_in_ref.at[pl.ds(c * PER_CHUNK, PER_CHUNK)]
        landed(counts, cnt_recv.at[c])
        slots = pl.ds(pl.multiple_of(c * SLOTS, SLOTS), SLOTS)
        fill_owners(counts[...], mask_ref)
        landed(recv_ref.at[:, slots, :], data_recv.at[c])
        for p in range(PAIRS):
            plain_step(p, recv_ref[p, slots, :], mask_ref, q_ref, acc_ref)
        return carry

    lax.fori_loop(0, CHUNKS, chunk_step, 0)

    others = pl.ds(0, DEVS - 1)
    landed(send_ref.at[others], data_send)
    landed(cnt_ref.at[others], cnt_send)
    landed(ids_ref.at[pl.ds(0, 7)], line_send)
    landed(ids_ref.at[pl.ds(0, 120)], plane_send)


def finish(sums_ref, hid_ref, w_in_ref, w_out_ref, stage_ref, out_hbm, sems):
    copies = []
    for p in range(PAIRS):
        share = sums_ref[p, 0:HEAD, :] * (1.0 / sums_ref[p, HEAD:HEAD + 1, :])
        users = []
        for v in range(2):
            starts = [v * USER + h * ROWS for h in range(HEADS)]
            tall = jnp.concatenate([share[:, lo:lo + ROWS] for lo in starts], axis=0)
            tall = jnp.concatenate([tall, jnp.zeros((WIDTH, 2 * WIDTH - ROWS), jnp.float32)], axis=1)
            users.append(tall.T[0:ROWS])
        interest = jnp.concatenate(users, axis=0).astype(jnp.bfloat16)
        hidden = jnp.dot(interest, w_in_ref[WIDTH:, :], preferred_element_type=jnp.float32)
        hidden = hidden + hid_ref[2 * p:2 * p + 2].reshape(2 * ROWS, HID)
        half = hidden * 0.5
        hidden = (half + half * jnp.tanh(half)).astype(jnp.bfloat16)
        result = jnp.dot(hidden, w_out_ref[...], preferred_element_type=jnp.float32).astype(jnp.bfloat16)
        stage_ref[2 * p:2 * p + 2] = result.reshape(2, ROWS, WIDTH)
        both = pl.ds(p * 2, 2)
        copies.append(pltpu.make_async_copy(stage_ref.at[both, 0:CANDS], out_hbm.at[both], sems.at[p]))
        copies[-1].start()
    for copy in copies:
        copy.wait()


def tower_kernel(acc_ref, cnt_ref, hid_ref, w_in_ref, w_out_ref, recv_hbm, cand_hbm, out_hbm,
                 stage_ref, again_ref, recv_ref, cand_ref, q_ref, mask_ref, top_ref, sems):
    finish(acc_ref, hid_ref, w_in_ref, w_out_ref, stage_ref, out_hbm, sems)
    weights = acc_ref[:, HEAD:HEAD + 1, :]
    good = (weights > 2.0 ** -80) & (weights < 2.0 ** 110)

    @pl.when(jnp.min(jnp.where(good, 1.0, 0.0)) < 0.5)
    def _():
        pltpu.sync_copy(recv_hbm, recv_ref)
        pltpu.sync_copy(cand_hbm, cand_ref)
        fill_queries(cand_ref, q_ref)
        top_ref[...] = jnp.full_like(top_ref, -3e38)
        again_ref[...] = jnp.zeros_like(again_ref)

        def chunk_step(c, carry):
            fill_owners(cnt_ref[pl.ds(pl.multiple_of(c * PER_CHUNK, PER_CHUNK), PER_CHUNK), :], mask_ref)

            def one(p, carry):
                keys = recv_ref[p, pl.ds(pl.multiple_of(c * SLOTS, SLOTS), SLOTS), :]
                shifted_step(p, keys, mask_ref, q_ref, top_ref, again_ref)
                return carry

            return lax.fori_loop(0, PAIRS, one, carry)

        lax.fori_loop(0, CHUNKS, chunk_step, 0)
        finish(again_ref, hid_ref, w_in_ref, w_out_ref, stage_ref, out_hbm, sems)


def local(history, event_cat, candidates, cand_cat, w_input, w_output):
    hist = history.transpose(1, 0, 2).reshape(E_DEV, DEVS, OWN, WIDTH)
    vm = pl.BlockSpec(memory_space=pltpu.VMEM)
    hbm = pl.BlockSpec(memory_space=pltpu.HBM)
    f32, bf16, dma = jnp.float32, jnp.bfloat16, pltpu.SemaphoreType.DMA
    sums, slots, counts, hidden = pl.pallas_call(
        exchange_kernel,
        out_shape=(
            jax.ShapeDtypeStruct((PAIRS, HEAD + 8, COLS), f32),
            jax.ShapeDtypeStruct((PAIRS, DEVS * CAP, WIDTH), bf16),
            jax.ShapeDtypeStruct((DEVS, WIDTH), f32),
            jax.ShapeDtypeStruct((OWN, ROWS, HID), f32),
        ),
        in_specs=[hbm] * 5,
        out_specs=(vm, vm, vm, vm),
        scratch_shapes=[
            pltpu.VMEM((E_DEV, DEVS * OWN), jnp.int32),
            pltpu.VMEM((OWN, CANDS), jnp.int32),
            pltpu.VMEM((OWN, CANDS, WIDTH), bf16),
            pltpu.VMEM((WIDTH, HID), bf16),
            pltpu.VMEM((32, DEVS * OWN), jnp.int32),
            pltpu.VMEM((DEVS * OWN, WIDTH), jnp.int32),
            pltpu.VMEM((DEVS, LANES), f32),
            pltpu.VMEM((DEVS, LANES, WIDTH), bf16),
            pltpu.VMEM((1, WIDTH), f32),
            pltpu.VMEM((DEVS, WIDTH), f32),
            pltpu.VMEM((DEVS, LANES), f32),
            pltpu.VMEM((DEVS, WIDTH), f32),
            pltpu.VMEM((DEVS, PAIRS, CAP, WIDTH), bf16),
            pltpu.VMEM((PAIRS, WIDTH, COLS), bf16),
            pltpu.VMEM((PAIRS, 3, SLOTS, WIDTH), bf16),
            pltpu.VMEM((WIDTH, LANES), bf16),
            pltpu.VMEM((LANES, LANES), bf16),
            pltpu.VMEM((LANES, WIDTH), bf16),
            dma((4,)), dma((E_DEV,)), dma, dma, dma, dma, dma, dma((CHUNKS,)), dma, dma((CHUNKS,)),
        ],
        compiler_params=pltpu.CompilerParams(collective_id=0, has_side_effects=True, vmem_limit_bytes=40 << 20),
        name="match_and_attend",
    )(*(pltpu.with_memory_space_constraint(x, pltpu.HBM) for x in (hist, event_cat.T, cand_cat, candidates, w_input)))
    return pl.pallas_call(
        tower_kernel,
        out_shape=jax.ShapeDtypeStruct((OWN, CANDS, WIDTH), bf16),
        in_specs=[vm] * 5 + [pl.BlockSpec(memory_space=pl.ANY)] * 2,
        out_specs=hbm,
        scratch_shapes=[
            pltpu.VMEM((OWN, ROWS, WIDTH), bf16),
            pltpu.VMEM((PAIRS, HEAD + 8, COLS), f32),
            pltpu.VMEM((PAIRS, DEVS * CAP, WIDTH), bf16),
            pltpu.VMEM((OWN, CANDS, WIDTH), bf16),
            pltpu.VMEM((PAIRS, WIDTH, COLS), bf16),
            pltpu.VMEM((PAIRS, 3, SLOTS, WIDTH), f32),
            pltpu.VMEM((PAIRS, 1, COLS), f32),
            dma((PAIRS,)),
        ],
        compiler_params=pltpu.CompilerParams(vmem_limit_bytes=40 << 20),
        name="tower",
    )(sums, counts, hidden, w_input, w_output, slots, candidates)


def solution(mesh):
    return jax.shard_map(
        local, mesh=mesh,
        in_specs=(P(None, AXES, None), P(None, AXES), P(AXES, None, None), P(AXES, None), P(), P()),
        out_specs=P(AXES, None, None), check_vma=False)
```
